32 devices in a mesh: section: 2 (over x), fsdp: 16 (over z, y, core).
Axes of the slice: x: 2, y: 2, z: 4, core: 2. Of those that a mesh axis runs over, the one named last changes fastest.
Arguments:
- tokens: bfloat16 [6, 512, 4096], P(None, 'fsdp'), may hold values from -6 to 6
- cotangent: bfloat16 [6, 512, 4096], P(None, 'fsdp'), may hold values from -6 to 6
- order: int32 [6], replicated, may hold values from 0 to 5, each once
- w_value: bfloat16 [2, 4096, 512], P('section', 'fsdp'), may hold values from -0.09375 to 0.09375
- w_out: bfloat16 [2, 512, 4096], P('section', None, 'fsdp'), may hold values from -0.25 to 0.25
- adapter_down: bfloat16 [2, 4096, 128], P('section', 'fsdp'), may hold values from -0.09375 to 0.09375
- adapter_up: bfloat16 [2, 128, 512], P('section', None, 'fsdp'), may hold values from -0.5 to 0.5
Outputs:
- input_grads: bfloat16 [2, 6, 512, 4096], P('section', None, 'fsdp')
- grad_down: float32 [2, 4096, 128], P('section', 'fsdp')
- grad_up: float32 [2, 128, 512], P('section', None, 'fsdp')
The draws below stay inside these ranges and needn't reach their ends.
Inputs may be any that keep to these rules, and one draw needn't show every extreme that they name: order names each microbatch 0 .. 5 exactly once.
All inputs are finite; a program needn't handle non-finite values.
Results may differ from the reference program's by a relative error of at most 0.02.
Values may be sent and summed in bfloat16 or wider, within the bound.
A program may use at most 128 MiB of HBM per device.

```python
import jax
import jax.numpy as jnp
from jax import lax

D = 4096
HV = 512
R = 128
MICRO = 6
MB = 512
SECTIONS = 2


def with_spikes(entries, own_key, source, target, blocks, factor):
    def block_of(dim):
        return (jnp.arange(entries.shape[dim]) // (entries.shape[dim] // blocks)).reshape((-1,) + (1,) * (entries.ndim - 1 - dim))

    near = jax.random.permutation(own_key, blocks)[block_of(target)]
    second = (block_of(target) + blocks // 2) % blocks
    return jnp.where((block_of(source) == near) | (block_of(source) == second), factor * entries, entries)


def level_of(own_key, dims, pieces, least, top_value):
    gain, own = 1.0, jax.random.fold_in(own_key, 6)
    for dim, blocks in pieces:
        draws = jnp.exp(jax.random.uniform(jax.random.fold_in(own, dim), (blocks,), jnp.float32, least / len(pieces), top_value / len(pieces)))
        gain = gain * jnp.repeat(draws, dims[dim] // blocks).reshape([-1 if axis == dim else 1 for axis in range(len(dims))])
    return gain


def noise(rng, extent, width, most, cuts=(), kind=jnp.bfloat16):
    gain = level_of(rng, extent, cuts, -0.22, 0.18) if cuts else 1.0
    entries = jax.random.normal(rng, extent, jnp.float32) * width * gain
    return jnp.minimum(jnp.maximum(entries, -most), most).astype(kind)


def heavy_noise(rng, shape, spread, bound, shards, heavy, held_as=jnp.bfloat16):
    array = spread * jax.random.normal(rng, shape, jnp.float32)
    if shards:
        array = array * level_of(rng, shape, shards, -0.22, 0.18)
    return jnp.clip(with_spikes(array, jax.random.fold_in(rng, 3), *heavy), -bound, bound).astype(held_as)


def setup_inputs(seed: int = 0) -> dict:
    streams_of = jax.random.split(jax.random.key(seed), 8)
    return {
        "tokens": heavy_noise(streams_of[0], (MICRO, MB, D), 1.0, 6.0, ((1, 16),), (1, 2, 16, 2.0)),
        "cotangent": heavy_noise(streams_of[1], (MICRO, MB, D), 1.0, 6.0, ((1, 16),), (1, 2, 16, 2.0)),
        "order": jax.random.permutation(streams_of[2], MICRO).astype(jnp.int32),
        "w_value": noise(streams_of[3], (SECTIONS, D, HV), D ** -0.5, 0.09375, ((0, 2), (1, 16))),
        "w_out": noise(streams_of[4], (SECTIONS, HV, D), HV ** -0.5, 0.25, ((0, 2), (2, 16))),
        "adapter_down": noise(streams_of[5], (SECTIONS, D, R), D ** -0.5, 0.09375, ((0, 2), (1, 16))),
        "adapter_up": noise(streams_of[6], (SECTIONS, R, HV), R ** -0.5, 0.5, ((0, 2), (2, 16))),
    }


epsilon = 1e-05

def layer_forward(inputs, w_val, w_proj, a_down, a_up):
    widened = inputs.astype(jnp.float32)
    inverse = lax.rsqrt(lax.optimization_barrier(jnp.mean(widened * widened, axis=-1, keepdims=True)) + epsilon)
    normed = (widened * inverse).astype(jnp.bfloat16)
    low = jnp.dot(normed, a_down, preferred_element_type=jnp.float32).astype(jnp.bfloat16)
    values = (jnp.dot(normed, w_val, preferred_element_type=jnp.float32) + jnp.dot(low, a_up, preferred_element_type=jnp.float32)).astype(jnp.bfloat16)
    outputs = (widened + jnp.dot(values, w_proj, preferred_element_type=jnp.float32)).astype(jnp.bfloat16)
    return (outputs, normed, low, inverse)

def layer_backward(inputs, inverse, upstream, w_val, w_proj, a_down, a_up):
    d_values = jnp.dot(upstream, w_proj.T, preferred_element_type=jnp.float32).astype(jnp.bfloat16)
    d_low = jnp.dot(d_values, a_up.T, preferred_element_type=jnp.float32).astype(jnp.bfloat16)
    d_normed = jnp.dot(d_values, w_val.T, preferred_element_type=jnp.float32) + jnp.dot(d_low, a_down.T, preferred_element_type=jnp.float32)
    widened = inputs.astype(jnp.float32)
    project = lax.optimization_barrier(jnp.mean(d_normed * widened, axis=-1, keepdims=True))
    d_inputs = upstream.astype(jnp.float32) + inverse * (d_normed - widened * inverse * inverse * project)
    return (d_inputs.astype(jnp.bfloat16), d_values, d_low)

def reference(tokens, cotangent, order, w_value, w_out, adapter_down, adapter_up):
    current = tokens[order].reshape(MICRO * MB, D)
    stored = []
    for section_index in range(SECTIONS):
        stored.append(current)
        current = layer_forward(current, w_value[section_index], w_out[section_index], adapter_down[section_index], adapter_up[section_index])[0]
    upstream = cotangent[order].reshape(MICRO * MB, D)
    grads_in = [None] * SECTIONS
    down_grads = [None] * SECTIONS
    up_grads = [None] * SECTIONS
    for section_index in reversed(range(SECTIONS)):
        inputs = stored[section_index]
        unused, normed, low, inverse = layer_forward(inputs, w_value[section_index], w_out[section_index], adapter_down[section_index], adapter_up[section_index])
        d_inputs, d_values, d_low = layer_backward(inputs, inverse, upstream, w_value[section_index], w_out[section_index], adapter_down[section_index], adapter_up[section_index])
        down_grads[section_index] = jnp.dot(normed.T, d_low, preferred_element_type=jnp.float32)
        up_grads[section_index] = jnp.dot(low.T, d_values, preferred_element_type=jnp.float32)
        grads_in[section_index] = d_inputs.reshape(MICRO, MB, D)
        upstream = d_inputs
    return (jnp.stack(grads_in), jnp.stack(down_grads), jnp.stack(up_grads))
```

```python
import functools

import jax
import jax.numpy as jnp
from jax import lax
from jax.experimental import pallas as pl
from jax.experimental.pallas import tpu as pltpu
from jax.sharding import PartitionSpec as P

epsilon = 1e-05
MESH = pl.DeviceIdType.MESH
X, Y, Z = 0, 1, 2
OUT, MIX, UP = 0, 1, 2
bf16, f32 = jnp.bfloat16, jnp.float32


def widen_dot(left, right, dims=((1,), (0,))):
    return lax.dot_general(left, right, (dims, ((), ())), preferred_element_type=f32)


def plan_of(out_rows, mix_rows, up_rows):
    out_y, mix_y, mix_x = out_rows * 3 // 16, mix_rows // 8, mix_rows // 4
    out_z, mix_z = (out_rows - out_y) // 2, (mix_rows - mix_y - mix_x) // 2
    return (
        (UP, 0, up_rows, (Z, Y)),
        (OUT, 0, out_z, (Z, Y, X)),
        (OUT, 2 * out_z, out_y, (Y, Z, X)),
        (OUT, out_z, out_z, (Z, Y, X)),
        (MIX, 0, mix_z, (Z, Y, X)),
        (MIX, mix_z, mix_z, (Z, Y, X)),
        (MIX, 2 * mix_z, mix_y, (Y, Z, X)),
        (MIX, 2 * mix_z + mix_y, mix_x, (X, Z, Y)),
    )


def relay_kernel(
    lines, plan, tok_any, cot_any, value_any, down_any, out_any, up_any, flow_any, grad_any,
    mix, out, up, tok, cot, normed, states, wide, flow, acc, vals, cats, tail, low, squares, products, scales,
    parts, near, mine, far, total,
    local_sem, recv_sem, send_sem, swap_recv, swap_send, near_recv, near_send, far_recv, far_send,
):
    pieces = len(plan)
    rows, features = tok.shape
    width = vals.shape[1]
    fsdp = lines * 4
    chips = lines * 2
    block = features // fsdp
    sheet = block * 4
    share_up = up.shape[1]
    s, f = lax.axis_index("section"), lax.axis_index("fsdp")
    core, y, z = f % 2, (f // 2) % 2, f // 4
    chip = f // 2
    first, second = s == 0, s == 1

    def place(s_, z_, y_, c_):
        return {"section": s_, "fsdp": (z_ * 2 + y_) * 2 + c_}

    partner = place(s, z, y, 1 - core)
    across = place(1 - s, z, y, core)
    beside = place(s, z, 1 - y, core)
    above = place(s, z + 1, y, core)
    below = place(s, z - 1, y, core)

    def stage(source, target, index):
        copy = pltpu.make_async_copy(source, target, local_sem.at[index])
        copy.start()
        return copy

    def band(slot, start, count):
        return pl.ds(pl.multiple_of(slot * block + start, 16), count)

    staged = {
        UP: [stage(up_any, up.at[f], 0)],
        OUT: [stage(out_any, out.at[s, f], 1)],
        MIX: [
            stage(value_any, mix.at[s, band(f, 0, block), :width], 2),
            stage(down_any, mix.at[s, band(f, 0, block), width:], 3),
        ],
    }
    tok_copy, cot_copy = stage(tok_any, tok, 4), stage(cot_any, cot, 5)

    barrier = pltpu.get_barrier_semaphore()
    for target in (partner, across):
        pl.semaphore_signal(barrier, inc=1, device_id=target, device_id_type=MESH)
    for step in range(1, chips):
        target = {"section": s, "fsdp": ((chip + step) % chips) * 2 + core}
        pl.semaphore_signal(barrier, inc=1, device_id=target, device_id_type=MESH)
    pl.semaphore_wait(barrier, chips + 1)

    def when(test, action):
        if test is True:
            action()
        else:
            pl.when(test)(action)

    def both(left, right):
        return right if left is True else left if right is True else left & right

    def slot_of(dy, dz, c_):
        return ((z + dz) * 2 + (y + dy) % 2) * 2 + c_

    def piece(index, owner, slot):
        array, start, count, _ = plan[index]
        if array == MIX:
            return mix.at[owner, band(slot, start, count), :]
        if array == OUT:
            return out.at[owner, slot, pl.ds(start, count)]
        return up.at[slot, pl.ds(start, count)]

    def inside(dz):
        return True if dz == 0 else (z + dz < lines) if dz > 0 else (z + dz >= 0)

    def gets(index, dx):
        if not dx:
            return True
        return first if plan[index][0] == MIX else second

    def gives(index):
        return second if plan[index][0] == MIX else first

    def sem_of(index, dx, slot):
        return recv_sem.at[(dx * fsdp + slot) * pieces + index]

    def sends(index, dx, dy, dz):
        order = plan[index][3]
        slot, owner = slot_of(dy, dz, core), (s + dx) % 2
        step = ((dx * 2 + dy) * lines + dz % lines) * pieces + index
        gone = {X: dx != 0, Y: dy != 0, Z: dz != 0}
        here = piece(index, owner, slot)
        result = []

        def add(way, test, target, hop=0):
            copy = pltpu.make_async_remote_copy(
                src_ref=here,
                dst_ref=here,
                send_sem=send_sem.at[step * 5 + way],
                recv_sem=sem_of(index, (dx + hop) % 2, slot),
                device_id=target,
                device_id_type=MESH,
            )
            result.append((test, copy))

        for rank, dim in enumerate(order):
            if any(gone[later] for later in order[rank + 1:]):
                continue
            if dim == Z:
                if dz <= 0:
                    add(0, z + 1 < lines, above)
                if dz >= 0:
                    add(1, z > 0, below)
            elif dim == Y and not gone[Y]:
                add(2, True, beside)
            elif dim == X and not gone[X]:
                add(3, gives(index), across, 1)
        add(4, True, partner)
        return result

    def arrived(index, dx, slot):
        ref = piece(index, (s + dx) % 2, slot)
        pltpu.make_async_copy(ref, ref, sem_of(index, dx, slot)).wait()

    levels = {}
    for dx in (0, 1):
        for dy in (0, 1):
            for dz in range(1 - lines, lines):
                for index in range(pieces):
                    if X in plan[index][3] or not dx:
                        levels.setdefault(dx + dy + abs(dz), []).append((index, dx, abs(dz), dy, dz))
    for level in levels.values():
        level.sort()
    of = {array: [index for index in range(pieces) if plan[index][0] == array] for array in (OUT, MIX, UP)}

    def relay(index, dx, dy, dz):
        def action():
            if dx or dy or dz:
                arrived(index, dx, slot_of(dy, dz, core))
            else:
                for copy in staged.pop(plan[index][0], ()):
                    copy.wait()
            for test, copy in sends(index, dx, dy, dz):
                when(test, copy.start)

        when(both(inside(dz), gets(index, dx)), action)

    def level_relays(distance):
        for index, dx, _, dy, dz in levels[distance]:
            relay(index, dx, dy, dz)

    turned = z // (lines // 2)
    folded = z + turned * (lines - 1 - 2 * z)

    def plane_of(rank):
        near_plane = folded if rank == 0 else 1 - folded if rank == 1 else rank
        return near_plane + turned * (lines - 1 - 2 * near_plane)

    def partners_arrived(array, dx, plane):
        for y_ in (0, 1):
            for index in of[array]:
                arrived(index, dx, (plane * 2 + y_) * 2 + 1 - core)

    def columns(index, count):
        return pl.ds(pl.multiple_of(index * count, count), count)

    def fold(product):
        sums = product[:, :128]
        for start in range(128, product.shape[1], 128):
            sums = sums + product[:, start:start + 128]
        return sums

    step = width

    def blocks(action, size=step):
        def run(index, carry):
            action(index)
            return carry

        lax.fori_loop(0, features // size, run, 0)

    def mean_of(sums):
        return jnp.sum(sums[...], axis=1, keepdims=True) / features

    level_relays(0)
    acc[...] = jnp.zeros_like(acc)
    squares[...] = jnp.zeros_like(squares)
    tok_copy.wait()
    cot_copy.wait()

    @pl.when(first)
    def _():
        def square(index):
            entries = tok[:, columns(index, step)].astype(f32)
            squares[...] += fold(entries * entries)

        blocks(square)
        inverse = lax.rsqrt(mean_of(squares) + epsilon)

        def scale(index):
            span = columns(index, step)
            normed[:, span] = (tok[:, span].astype(f32) * inverse).astype(bf16)

        blocks(scale)
        scales[...] = jnp.broadcast_to(inverse, scales.shape)

    for rank in range(lines):
        level_relays(rank + 1)
        plane = plane_of(rank)

        @pl.when(first)
        def _():
            partners_arrived(MIX, 0, plane)
            span = columns(plane, sheet)
            acc[...] += widen_dot(normed[:, span], mix[0, span, :])

        @pl.when(second)
        def _():
            partners_arrived(OUT, 0, plane)
            sums = acc[:, :width]
            for part in range(4):
                span = pl.ds(pl.multiple_of(plane * sheet + part * block, block), block)
                sums = sums + widen_dot(cot[:, span], out[1, plane * 4 + part], ((1,), (1,)))
            acc[:, :width] = sums

    for plane in range(lines):
        partners_arrived(UP, 0, plane)

    def swap(ref, index):
        return pltpu.make_async_remote_copy(
            src_ref=ref,
            dst_ref=ref,
            send_sem=swap_send.at[index],
            recv_sem=swap_recv.at[index],
            device_id=across,
            device_id_type=MESH,
        )

    def ups():
        return up[...].reshape(fsdp * share_up, up.shape[2])

    @pl.when(first)
    def _():
        low[...] = acc[:, width:].astype(bf16)
        vals[...] = (acc[:, :width] + widen_dot(low[...], ups(), ((1,), (1,)))).astype(bf16)
        swap(vals, 0).start()

    @pl.when(second)
    def _():
        cats[:, :width] = acc[:, :width].astype(bf16)
        cats[:, width:] = widen_dot(cats[:, :width], ups()).astype(bf16)
        swap(cats, 1).start()

    level_relays(lines + 1)

    @pl.when(first)
    def _():
        for plane in range(lines):
            partners_arrived(OUT, 0, plane)

    @pl.when(second)
    def _():
        for plane in range(lines):
            partners_arrived(OUT, 1, plane)
        swap(vals, 0).wait_recv()

    squares[...] = jnp.zeros_like(squares)
    products[...] = jnp.zeros_like(products)

    def widen(index):
        span = columns(index, block)
        entries = (tok[:, span].astype(f32) + widen_dot(vals[...], out[0, index])).astype(bf16)
        states[:, span] = entries
        back = entries.astype(f32)
        squares[...] += fold(back * back)

    blocks(widen, block)

    @pl.when(first)
    def _():
        for plane in range(lines):
            partners_arrived(MIX, 1, plane)
        swap(cats, 1).wait_recv()

    @pl.when(second)
    def _():
        for plane in range(lines):
            partners_arrived(MIX, 0, plane)

    def open_up(layer, joint, inputs):
        def action(index):
            span = columns(index, step)
            entries = widen_dot(joint[...], mix[layer, span, :], ((1,), (1,)))
            wide[:, span] = entries
            products[...] += fold(entries * inputs[:, span].astype(f32))

        blocks(action)

    open_up(1, cats, states)
    inverse = lax.rsqrt(mean_of(squares) + epsilon)
    factor = inverse * inverse * mean_of(products)
    acc[...] = jnp.zeros_like(acc)

    def gradients(joint):
        def contract(index, carry):
            parts[index // 2, index % 2, :block, :] = widen_dot(
                normed[:, columns(index, block)], joint[:, width:], ((0,), (0,))
            ).astype(bf16)
            return carry

        lax.fori_loop(0, fsdp, contract, 0)
        ends = widen_dot(joint[:, :width], low[...], ((0,), (0,))).astype(bf16)
        for index in range(fsdp):
            parts[index // 2, index % 2, block:, :] = ends[index * share_up:(index + 1) * share_up]

    def upstream_of(span):
        inputs = states[:, span].astype(f32)
        entries = cot[:, span].astype(f32) + inverse * (wide[:, span] - inputs * factor)
        flow[:, span] = entries.astype(bf16)
        return inputs

    @pl.when(first)
    def _():
        def narrow(index):
            span = columns(index, block)
            upstream_of(span)
            acc[:, :width] += widen_dot(flow[:, span], out[0, index], ((1,), (1,)))

        blocks(narrow, block)
        tail[:, :width] = acc[:, :width].astype(bf16)
        tail[:, width:] = widen_dot(tail[:, :width], ups()).astype(bf16)
        gradients(tail)

    @pl.when(second)
    def _():
        def lower(index):
            span = columns(index, step)
            inputs = upstream_of(span)
            normed[:, span] = (inputs * inverse).astype(bf16)
            acc[:, width:] += widen_dot(normed[:, span], mix[1, span, width:])

        blocks(lower)
        low[...] = acc[:, width:].astype(bf16)
        gradients(cats)

    handed, passed = [], []
    for turn in range(chips):
        target = (chip + 1 + turn) % chips
        copy = pltpu.make_async_remote_copy(
            src_ref=parts.at[target, 1 - core],
            dst_ref=near.at[turn],
            send_sem=near_send.at[turn],
            recv_sem=near_recv.at[turn],
            device_id=partner,
            device_id_type=MESH,
        )
        copy.start()
        handed.append(copy)
    for turn in range(chips - 1):
        target = (chip + 1 + turn) % chips
        handed[turn].wait_recv()
        mine[turn] = (parts[target, core].astype(f32) + near[turn].astype(f32)).astype(bf16)
        copy = pltpu.make_async_remote_copy(
            src_ref=mine.at[turn],
            dst_ref=far.at[turn],
            send_sem=far_send.at[turn],
            recv_sem=far_recv.at[turn],
            device_id={"section": s, "fsdp": target * 2 + core},
            device_id_type=MESH,
        )
        passed.append(copy)
        if turn:
            passed[turn - 1].start()
    handed[-1].wait_recv()
    total[...] = parts[chip, core].astype(f32) + near[chips - 1].astype(f32)
    passed[-1].start()

    @pl.when(first)
    def _():
        products[...] = jnp.zeros_like(products)
        open_up(0, tail, tok)
        inverse = scales[:, :1]
        factor = inverse * inverse * mean_of(products)

        def finish(index):
            span = columns(index, step)
            entries = flow[:, span].astype(f32) + inverse * (wide[:, span] - tok[:, span].astype(f32) * factor)
            flow[:, span] = entries.astype(bf16)

        blocks(finish)

    flow_copy = pltpu.make_async_copy(flow, flow_any, local_sem.at[0])
    flow_copy.start()
    for turn in range(chips - 1):
        passed[turn].wait_recv()
        total[...] += far[turn].astype(f32)
    grad_copy = pltpu.make_async_copy(total, grad_any, local_sem.at[1])
    grad_copy.start()
    for distance in sorted(levels):
        for index, dx, _, dy, dz in levels[distance]:
            for test, copy in sends(index, dx, dy, dz):
                when(both(both(inside(dz), gets(index, dx)), test), copy.wait_send)
    pl.when(first)(swap(vals, 0).wait_send)
    pl.when(second)(swap(cats, 1).wait_send)
    for copy in handed + passed:
        copy.wait_send()
    flow_copy.wait()
    grad_copy.wait()


def finish_kernel(micro, order_ref, flow_ref, grad_ref, out_ref, down_ref, up_ref):
    local = flow_ref.shape[0] // micro
    for slot in range(micro):
        out_ref[slot] = flow_ref[pl.ds(pl.multiple_of(order_ref[slot] * local, local), local), :]
    split = down_ref.shape[0]
    down_ref[...] = grad_ref[:split]
    up_ref[...] = grad_ref[split:]


def custom_route():
    fsdp = lax.axis_size("fsdp")
    return lax.axis_size("section") == 2 and fsdp % 8 == 0 and fsdp <= 16


def run_custom(tokens, cotangent, order, value, down, out, up):
    micro, local, features = tokens.shape
    rows = micro * local
    fsdp = lax.axis_size("fsdp")
    lines, chips = fsdp // 4, fsdp // 2
    block, width = value.shape
    rank = down.shape[1]
    share_up = up.shape[0]
    both, high = width + rank, block + share_up
    plan = plan_of(width, block, share_up)
    pieces = len(plan)
    outside, inside = pl.BlockSpec(memory_space=pl.ANY), pl.BlockSpec(memory_space=pltpu.VMEM)
    dma = pltpu.SemaphoreType.DMA
    vmem = pltpu.VMEM
    flow, grads = pl.pallas_call(
        functools.partial(relay_kernel, lines, plan),
        out_shape=[
            jax.ShapeDtypeStruct((rows, features), bf16),
            jax.ShapeDtypeStruct((high, rank), f32),
        ],
        in_specs=[outside] * 6,
        out_specs=[outside] * 2,
        scratch_shapes=[
            vmem((2, features, both), bf16),
            vmem((2, fsdp, width, block), bf16),
            vmem((fsdp, share_up, rank), bf16),
            vmem((rows, features), bf16),
            vmem((rows, features), bf16),
            vmem((rows, features), bf16),
            vmem((rows, features), bf16),
            vmem((rows, features), f32),
            vmem((rows, features), bf16),
            vmem((rows, both), f32),
            vmem((rows, width), bf16),
            vmem((rows, both), bf16),
            vmem((rows, both), bf16),
            vmem((rows, rank), bf16),
            vmem((rows, 128), f32),
            vmem((rows, 128), f32),
            vmem((rows, 128), f32),
            vmem((chips, 2, high, rank), bf16),
            vmem((chips, high, rank), bf16),
            vmem((chips, high, rank), bf16),
            vmem((chips, high, rank), bf16),
            vmem((high, rank), f32),
            dma((6,)),
            dma((2 * fsdp * pieces,)),
            dma((fsdp * pieces * 5,)),
            dma((2,)),
            dma((2,)),
            dma((chips,)),
            dma((chips,)),
            dma((chips,)),
            dma((chips,)),
        ],
        compiler_params=pltpu.CompilerParams(
            collective_id=0, has_side_effects=True, vmem_limit_bytes=52 * 2**20
        ),
    )(tokens.reshape(rows, features), cotangent.reshape(rows, features), value, down, out, up)
    return pl.pallas_call(
        functools.partial(finish_kernel, micro),
        out_shape=[
            jax.ShapeDtypeStruct((micro, local, features), bf16),
            jax.ShapeDtypeStruct((block, rank), f32),
            jax.ShapeDtypeStruct((share_up, rank), f32),
        ],
        in_specs=[pl.BlockSpec(memory_space=pltpu.SMEM), inside, inside],
        out_specs=[inside] * 3,
    )(order, flow, grads)


def gather_weights(w_value, w_out, adapter_down, adapter_up):
    sections = lax.axis_size("section")

    def whole(block):
        full = lax.all_gather(block, ("section", "fsdp"), axis=0, tiled=True)
        return full.reshape(sections, -1, block.shape[1])

    joined = jnp.concatenate([w_value[0], adapter_down[0]], axis=1)
    return whole(joined), whole(w_out[0].T), whole(adapter_up[0].T)


def body(tokens, cotangent, order, w_value, w_out, adapter_down, adapter_up):
    sections = lax.axis_size("section")
    position = lax.axis_index("section")
    micro, local, features = tokens.shape
    width = w_value.shape[2]

    if custom_route():
        out, grad_down, grad_up = run_custom(
            tokens, cotangent, order, w_value[0], adapter_down[0], w_out[0], adapter_up[0].T
        )
        return (out[None], grad_down[None], grad_up.T[None])

    joined, proj, up = gather_weights(w_value, w_out, adapter_down, adapter_up)
    current = tokens.reshape(micro * local, features)
    saved = []
    for layer in range(sections):
        widened = current.astype(jnp.float32)
        inverse = lax.rsqrt(jnp.mean(widened * widened, axis=-1, keepdims=True) + epsilon)
        normed = (widened * inverse).astype(jnp.bfloat16)
        last = layer == sections - 1
        if last:
            low = widen_dot(normed, joined[layer][:, width:]).astype(jnp.bfloat16)
        else:
            both = widen_dot(normed, joined[layer])
            low = both[:, width:].astype(jnp.bfloat16)
            values = (both[:, :width] + widen_dot(low, up[layer], ((1,), (1,)))).astype(jnp.bfloat16)
        saved.append((current, normed, low, inverse))
        if not last:
            current = (widened + widen_dot(values, proj[layer], ((1,), (1,)))).astype(jnp.bfloat16)

    upstream = cotangent.reshape(micro * local, features)
    grads, d_vals, d_lows = [], [], []
    for layer in reversed(range(sections)):
        inputs, normed, low, inverse = saved[layer]
        d_values = widen_dot(upstream, proj[layer]).astype(jnp.bfloat16)
        d_low = widen_dot(d_values, up[layer]).astype(jnp.bfloat16)
        d_normed = widen_dot(
            jnp.concatenate([d_values, d_low], axis=1), joined[layer], ((1,), (1,))
        )
        widened = inputs.astype(jnp.float32)
        project = jnp.mean(d_normed * widened, axis=-1, keepdims=True)
        upstream = (
            upstream.astype(jnp.float32)
            + inverse * (d_normed - widened * inverse * inverse * project)
        ).astype(jnp.bfloat16)
        grads.insert(0, upstream)
        d_vals.insert(0, d_values)
        d_lows.insert(0, d_low)

    def mine(items):
        chosen = items[0]
        for layer in range(1, sections):
            chosen = jnp.where(position == layer, items[layer], chosen)
        return chosen

    shares = lax.axis_size("fsdp")
    normed = mine([item[1] for item in saved])
    low = mine([item[2] for item in saved])
    part_down = widen_dot(normed, mine(d_lows), ((0,), (0,)))
    part_up = widen_dot(mine(d_vals), low, ((0,), (0,)))
    rank = low.shape[1]
    parts = jnp.concatenate(
        [part_down.reshape(shares, -1, rank), part_up.reshape(shares, -1, rank)], axis=1
    )
    share_down = features // shares
    combined = lax.psum_scatter(parts, "fsdp", scatter_dimension=0, tiled=True)[0]
    grad_down, grad_up = combined[:share_down], combined[share_down:]
    out = mine(grads).reshape(micro, local, features)[order]
    return (out[None], grad_down[None], grad_up.T[None])


def solution(mesh):
    return jax.shard_map(
        body,
        mesh=mesh,
        in_specs=(
            P(None, "fsdp", None),
            P(None, "fsdp", None),
            P(),
            P("section", "fsdp", None),
            P("section", None, "fsdp"),
            P("section", "fsdp", None),
            P("section", None, "fsdp"),
        ),
        out_specs=(
            P("section", None, "fsdp", None),
            P("section", "fsdp", None),
            P("section", None, "fsdp"),
        ),
        check_vma=False,
    )
```

```python
import functools

import jax
import jax.numpy as jnp
from jax import lax
from jax.experimental import pallas as pl
from jax.experimental.pallas import tpu as pltpu
from jax.sharding import PartitionSpec as P

epsilon = 1e-05
MESH = pl.DeviceIdType.MESH
X, Y, Z = 0, 1, 2
OUT, MIX, UP = 0, 1, 2
bf16, f32 = jnp.bfloat16, jnp.float32


def widen_dot(left, right, dims=((1,), (0,))):
    return lax.dot_general(left, right, (dims, ((), ())), preferred_element_type=f32)


def plan_of(out_rows, mix_rows, up_rows):
    def cut(array, rows, shares):
        start, result = 0, []
        for share, order, late in shares:
            count = rows * share // 32
            result.append((array, start, count, order, late))
            start += count
        return result

    none = ((0, 0), (0, 0))
    return tuple(
        cut(UP, up_rows, [(32, (Z, Y), none)])
        + cut(OUT, out_rows, [
                (7, (Z, Y, X), ((-0.25, -1.0), (-0.25, 2.0))),
                (10, (Z, Y, X), ((0, 0.25), (0, 0.0))),
                (8, (Y, Z, X), ((0.5, 0), (-0.75, 1.25))),
                (7, (X, Z, Y), ((2, -1.5), (0.25, 1.75))),
            ])
        + cut(MIX, mix_rows, [
                (8, (Z, Y, X), ((-0.5, 2.5), (0.75, 1.25))),
                (16, (Z, Y, X), ((0.25, -0.5), (-1, 0.75))),
                (4, (X, Z, Y), ((0, 1.5), (1.5, 2.0))),
                (4, (X, Y, Z), ((-0.25, 2), (2, -1))),
            ])
    )


def relay_kernel(
    lines, plan, tok_any, cot_any, value_any, down_any, out_any, up_any, flow_any, grad_any,
    mix, out, up, tok, cot, normed, states, wide, flow, acc, vals, cats, tail, low, squares, products, scales,
    parts, near, mine, beside_sums, sent, far, total,
    local_sem, recv_sem, send_sem, swap_sem, near_sem, side_sem, far_sem,
):
    pieces = len(plan)
    rows, features = tok.shape
    width, rank = vals.shape[1], low.shape[1]
    fsdp, chips = lines * 4, lines * 2
    block = features // fsdp
    sheet = block * 4
    share_up = up.shape[0] // fsdp
    high = {UP: share_up, OUT: width, MIX: block}
    count_of = {array: sum(item[0] == array for item in plan) for array in high}
    lead = {array: min(index for index in range(pieces) if plan[index][0] == array) for array in high}
    kinds = pieces + max(count_of[OUT], count_of[MIX])
    s, f = lax.axis_index("section"), lax.axis_index("fsdp")
    core, y, z = f % 2, (f // 2) % 2, f // 4
    chip = f // 2

    def place(s_, z_, y_, c_):
        return {"section": s_, "fsdp": (z_ * 2 + y_) * 2 + c_}

    partner = place(s, z, y, 1 - core)
    across = place(1 - s, z, y, core)
    beside = place(s, z, 1 - y, core)
    above = place(s, z + 1, y, core)
    below = place(s, z - 1, y, core)

    def stage(source, target, index):
        copy = pltpu.make_async_copy(source, target, local_sem.at[index])
        copy.start()
        return copy

    def band(array, slot, start, count):
        return pl.ds(pl.multiple_of(slot * high[array] + start, 16), count)

    staged = {
        UP: [stage(up_any, up.at[band(UP, f, 0, share_up), :], 0)],
        OUT: [stage(out_any, out.at[s, band(OUT, f, 0, width), :], 1)],
        MIX: [
            stage(value_any, mix.at[s, band(MIX, f, 0, block), :width], 2),
            stage(down_any, mix.at[s, band(MIX, f, 0, block), width:], 3),
        ],
    }
    inputs_staged = [stage(tok_any, tok, 4), stage(cot_any, cot, 5)]

    barrier = pltpu.get_barrier_semaphore()
    for target in (partner, across):
        pl.semaphore_signal(barrier, inc=1, device_id=target, device_id_type=MESH)
    for step in range(1, chips):
        target = {"section": s, "fsdp": ((chip + step) % chips) * 2 + core}
        pl.semaphore_signal(barrier, inc=1, device_id=target, device_id_type=MESH)
    pl.semaphore_wait(barrier, chips + 1)
    for array in (UP, OUT, MIX):
        for copy in staged[array]:
            copy.wait()

    def when(test, action):
        if test is True:
            action()
        else:
            pl.when(test)(action)

    def both(left, right):
        return right if left is True else left if right is True else left & right

    def slot_of(dy, dz, c_):
        return ((z + dz) * 2 + (y + dy) % 2) * 2 + c_

    def held(array, owner, span):
        return up.at[span, :] if array == UP else (mix if array == MIX else out).at[owner, span, :]

    def piece(index, owner, slot):
        array, start, count = plan[index][:3]
        return held(array, owner, band(array, slot, start, count))

    def whole(array, owner, slot):
        return held(array, owner, band(array, slot, 0, high[array]))

    def inside(dz):
        return True if dz == 0 else (z + dz < lines) if dz > 0 else (z + dz >= 0)

    def sem_of(index, dx, slot):
        kind = pieces + index - lead[plan[index][0]] if dx else index
        return recv_sem.at[slot // 2 * (kinds + 4) + kind]

    def whole_sem(array, dx, slot):
        return recv_sem.at[slot // 2 * (kinds + 4) + kinds + (3 if dx else array)]

    turned = z // (lines // 2)
    folded = z + turned * (lines - 1 - 2 * z)

    def plane_of(reach):
        near_plane = folded if reach == 0 else 1 - folded if reach == 1 else reach
        return near_plane + turned * (lines - 1 - 2 * near_plane)

    def columns(index, count):
        return pl.ds(pl.multiple_of(index * count, count), count)

    def fold(product):
        sums = product[:, :128]
        for start in range(128, product.shape[1], 128):
            sums = sums + product[:, start:start + 128]
        return sums

    step = width

    def blocks(action, size=step):
        def run(index, carry):
            action(index)
            return carry

        lax.fori_loop(0, features // size, run, 0, unroll=4)

    def mean_of(sums):
        return jnp.sum(sums[...], axis=1, keepdims=True) / features

    def ups():
        return up[...]

    def block_of_out(owner, slot):
        return out[owner, band(OUT, slot, 0, width), :]

    def swap(ref):
        return pltpu.make_async_remote_copy(
            src_ref=ref,
            dst_ref=ref,
            send_sem=swap_sem.at[0],
            recv_sem=swap_sem.at[1],
            device_id=across,
            device_id_type=MESH,
        )

    acc[...] = jnp.zeros_like(acc)
    squares[...] = jnp.zeros_like(squares)
    products[...] = jnp.zeros_like(products)

    def program(sec):
        lone, common = (MIX, OUT) if sec == 0 else (OUT, MIX)

        def late(index, dx):
            return plan[index][4][sec][dx]

        def routes(index, dx, dy, dz):
            gone, result = {X: dx != 0, Y: dy != 0, Z: dz != 0}, []
            for turn, dim in enumerate(plan[index][3]):
                if any(gone[later] for later in plan[index][3][turn + 1:]):
                    continue
                if dim == Z:
                    result += [(Z, 1)] * (dz <= 0) + [(Z, -1)] * (dz >= 0)
                elif dim == Y and not gone[Y]:
                    result.append((Y, 1))
                elif dim == X and not gone[X] and plan[index][0] == common:
                    result.append((X, 1))
            return result

        def push(ref, array, way, target, sem):
            pltpu.make_async_remote_copy(
                src_ref=ref,
                dst_ref=ref,
                send_sem=send_sem.at[array * 4 + way],
                recv_sem=sem,
                device_id=target,
                device_id_type=MESH,
            ).start()

        def send_all(index, dx, dy, dz):
            slot, array = slot_of(dy, dz, core), plan[index][0]
            here = piece(index, (sec + dx) % 2, slot)
            for dim, sign in routes(index, dx, dy, dz):
                target = {Y: beside, X: across}.get(dim, above if sign > 0 else below)
                test = True if dim != Z else z + 1 < lines if sign > 0 else z > 0
                sem = sem_of(index, 1 if dim == X else dx, slot)
                when(test, functools.partial(push, here, array, dim, target, sem))

        def arrived(index, dx, slot):
            ref = piece(index, (sec + dx) % 2, slot)
            pltpu.make_async_copy(ref, ref, sem_of(index, dx, slot)).wait()

        def partners_arrived(array, dx, plane):
            for y_ in (0, 1):
                slot = (plane * 2 + y_) * 2 + 1 - core
                ref = whole(array, (sec + dx) % 2, slot)
                pltpu.make_async_copy(ref, ref, whole_sem(array, dx, slot)).wait()

        events = []
        for dx in (0, 1):
            for dy in (0, 1):
                for dz in range(1 - lines, lines):
                    for index in range(pieces):
                        if not dx or plan[index][0] == lone:
                            key = dx + dy + abs(dz) + late(index, dx)
                            events.append((key, index, dx, abs(dz), dy, dz))
        events.sort()
        closing = {(plan[index][0], dx, dy, dz): number for number, (_, index, dx, _, dy, dz) in enumerate(events)}

        def relay(number, index, dx, dy, dz):
            array, slot = plan[index][0], slot_of(dy, dz, core)

            def action():
                if dx or dy or dz:
                    arrived(index, dx, slot)
                send_all(index, dx, dy, dz)
                if closing[array, dx, dy, dz] == number:
                    push(whole(array, (sec + dx) % 2, slot), array, 3, partner, whole_sem(array, dx, slot))

            when(inside(dz), action)

        def sent_rows(array, way, z_):
            rows_ = 0
            for _, index, dx, _, dy, dz in events:
                if plan[index][0] == array and 0 <= z_ + dz < lines:
                    for dim, sign in routes(index, dx, dy, dz):
                        if dim == way and (dim != Z or 0 <= z_ + sign < lines):
                            rows_ += plan[index][2]
            if way == 3:
                rows_ = high[array] * chips * (2 if array == lone else 1)
            return rows_

        def drain_sends():
            for array in high:
                for way in (X, Y, Z, 3):
                    for fold_ in range(lines // 2):
                        rows_ = sent_rows(array, way, fold_)
                        if not rows_ or (way != Z and fold_):
                            continue

                        def wait(rows_=rows_, array=array, way=way):
                            ref = held(array, 0, pl.ds(0, rows_))
                            pltpu.make_async_copy(ref, ref, send_sem.at[array * 4 + way]).wait()

                        when(folded == fold_ if way == Z else True, wait)

        def ready(array, dx, reach):
            return max(dx + 1 + reach + late(index, dx) for index in range(pieces) if plan[index][0] == array)

        def prepare():
            for copy in inputs_staged:
                copy.wait()
            if sec:
                return

            def square(index):
                entries = tok[:, columns(index, step)].astype(f32)
                squares[...] += fold(entries * entries)

            blocks(square)
            inverse = lax.rsqrt(mean_of(squares) + epsilon)

            def scale(index):
                span = columns(index, step)
                normed[:, span] = (tok[:, span].astype(f32) * inverse).astype(bf16)

            blocks(scale)
            scales[...] = jnp.broadcast_to(inverse, scales.shape)
            squares[...] = jnp.zeros_like(squares)

        def part_of(plane, part):
            return pl.ds(pl.multiple_of(plane * sheet + part * block, block), block)

        def lone_plane(reach):
            plane = plane_of(reach)
            partners_arrived(lone, 0, plane)
            if sec == 0:
                span = columns(plane, sheet)
                acc[...] += widen_dot(normed[:, span], mix[0, span, :])
                return
            sums = acc[:, :width]
            for part in range(4):
                sums = sums + widen_dot(cot[:, part_of(plane, part)], block_of_out(1, plane * 4 + part), ((1,), (1,)))
            acc[:, :width] = sums

        def emit():
            for plane in range(lines):
                partners_arrived(UP, 0, plane)
            if sec == 0:
                low[...] = acc[:, width:].astype(bf16)
                vals[...] = (acc[:, :width] + widen_dot(low[...], ups(), ((1,), (1,)))).astype(bf16)
                swap(vals).start()
            else:
                cats[:, :width] = acc[:, :width].astype(bf16)
                cats[:, width:] = widen_dot(cats[:, :width], ups()).astype(bf16)
                swap(cats).start()

        def widen(reach):
            plane = plane_of(reach)
            partners_arrived(OUT, sec, plane)
            for part in range(4):
                span = part_of(plane, part)
                added = widen_dot(vals[...], block_of_out(0, plane * 4 + part))
                entries = (tok[:, span].astype(f32) + added).astype(bf16)
                states[:, span] = entries
                back = entries.astype(f32)
                squares[...] += fold(back * back)
                if sec:
                    products[...] += fold(back * wide[:, span])

        def open_up(layer, joint, span, inputs):
            entries = widen_dot(joint[...], mix[layer, span, :], ((1,), (1,)))
            wide[:, span] = entries
            if inputs is not None:
                products[...] += fold(entries * inputs[:, span].astype(f32))

        def open_plane(reach):
            plane = plane_of(reach)
            partners_arrived(MIX, 1 - sec, plane)
            for part in range(2):
                span = pl.ds(pl.multiple_of(plane * sheet + part * step, step), step)
                open_up(1, cats, span, states if sec == 0 else None)

        def scoped(name, action, *args):
            with jax.named_scope(name):
                action(*args)

        timeline = [(key, 0, number, "relay%d" % int(key), functools.partial(relay, number, *event[:2], *event[3:]))
                    for number, (key, *event) in enumerate(events)]
        emitted = ready(lone, 0, lines - 1) + 0.02
        timeline.append((0.01, 1, 0, "prepare", prepare))
        timeline.append((emitted, 2, 0, "emit", emit))
        for reach in range(lines):
            timeline.append((ready(lone, 0, reach), 1, reach, "lone", functools.partial(lone_plane, reach)))
            early, behind = (widen, open_plane) if sec == 0 else (open_plane, widen)
            key = max(ready(common, 0, reach), emitted)
            timeline.append((key, 3, reach, early.__name__, functools.partial(early, reach)))
            timeline.append((1000, 2, reach, behind.__name__, functools.partial(behind, reach)))
        timeline.append((1000, 1, 0, "swapped", swap(vals).wait_recv if sec else swap(cats).wait_recv))
        timeline.sort(key=lambda item: item[:3])
        for _, _, _, name, action in timeline:
            scoped(name, action)

        def gradients(joint):
            turned_low = joint[:, width:].T
            for index in range(fsdp):
                product = widen_dot(turned_low, normed[:, index * block:(index + 1) * block]).astype(bf16)
                for start in range(0, block, rank):
                    parts[index % 2, index // 4, index // 2 % 2, start:start + rank, :] = product[:, start:start + rank]
            ends = widen_dot(joint[:, :width], low[...], ((0,), (0,))).astype(bf16)
            for index in range(fsdp):
                owned = ends[index * share_up:(index + 1) * share_up]
                parts[index % 2, index // 4, index // 2 % 2, block:, :] = owned

        handed, sided, passed = [], [], []
        half = lines // 2

        def settle():
            for turn in (0, 1):
                span = pl.ds((turned + 1 + turn) % 2 * half, half)
                copy = pltpu.make_async_remote_copy(
                    src_ref=parts.at[1 - core, span],
                    dst_ref=near.at[span],
                    send_sem=near_sem.at[2 + turn],
                    recv_sem=near_sem.at[turn],
                    device_id=partner,
                    device_id_type=MESH,
                )
                copy.start()
                handed.append(copy)
            for turn in range(lines):
                if turn % half == 0:
                    handed[turn // half].wait_recv()
                plane = plane_of(lines - 1 - turn)
                mine[plane] = (parts[core, plane, 1 - y].astype(f32) + near[plane, 1 - y].astype(f32)).astype(bf16)
                copy = pltpu.make_async_remote_copy(
                    src_ref=mine.at[plane],
                    dst_ref=beside_sums.at[plane],
                    send_sem=side_sem.at[lines + turn],
                    recv_sem=side_sem.at[turn],
                    device_id=beside,
                    device_id_type=MESH,
                )
                sided.append(copy)
                if turn:
                    sided[turn - 1].start()
            sided[-1].start()

        def pass_on():
            for turn in range(lines):
                sided[turn].wait_recv()
                plane = plane_of(lines - 1 - turn)
                sums = parts[core, plane, y].astype(f32) + near[plane, y].astype(f32) + beside_sums[plane].astype(f32)
                if turn == lines - 1:
                    total[...] = sums
                    continue
                sent[turn] = sums.astype(bf16)
                copy = pltpu.make_async_remote_copy(
                    src_ref=sent.at[turn],
                    dst_ref=far.at[z],
                    send_sem=far_sem.at[lines + turn],
                    recv_sem=far_sem.at[z],
                    device_id=place(s, plane, y, core),
                    device_id_type=MESH,
                )
                copy.start()
                passed.append(copy)

        def write_flow():
            copy = pltpu.make_async_copy(flow, flow_any, local_sem.at[0])
            copy.start()
            return copy

        inverse = lax.rsqrt(mean_of(squares) + epsilon)

        def upstream_of(span, factor):
            inputs = states[:, span].astype(f32)
            entries = cot[:, span].astype(f32) + inverse * (wide[:, span] - inputs * factor)
            flow[:, span] = entries.astype(bf16)

        acc[...] = jnp.zeros_like(acc)
        factor = inverse * inverse * mean_of(products)
        if sec == 0:
            def narrow(index):
                span = columns(index, block)
                upstream_of(span, factor)
                acc[:, :width] += widen_dot(flow[:, span], block_of_out(0, index), ((1,), (1,)))

            scoped("narrow", blocks, narrow, block)
            tail[:, :width] = acc[:, :width].astype(bf16)
            tail[:, width:] = widen_dot(tail[:, :width], ups()).astype(bf16)
            scoped("grads", gradients, tail)
            scoped("settle", settle)
            products[...] = jnp.zeros_like(products)
            scoped("open0", blocks, lambda index: open_up(0, tail, columns(index, step), tok))
            scoped("pass", pass_on)
            first_inverse = scales[:, :1]
            first_factor = first_inverse * first_inverse * mean_of(products)

            def finish(index):
                span = columns(index, step)
                change = wide[:, span] - tok[:, span].astype(f32) * first_factor
                flow[:, span] = (flow[:, span].astype(f32) + first_inverse * change).astype(bf16)

            scoped("finish", blocks, finish)
            flow_copy = write_flow()
        else:
            def lower(index):
                span = columns(index, step)
                normed[:, span] = (states[:, span].astype(f32) * inverse).astype(bf16)
                acc[:, width:] += widen_dot(normed[:, span], mix[1, span, width:])

            scoped("lower", blocks, lower)
            low[...] = acc[:, width:].astype(bf16)
            scoped("grads", gradients, cats)
            scoped("settle", settle)
            scoped("upstream", blocks, lambda index: upstream_of(columns(index, step), factor))
            flow_copy = write_flow()
            scoped("pass", pass_on)

        def settled():
            for reach in range(1, lines):
                plane = plane_of(reach)
                pltpu.make_async_copy(far.at[plane], far.at[plane], far_sem.at[plane]).wait()
                total[...] += far[plane].astype(f32)

        scoped("settled", settled)
        grad_copy = pltpu.make_async_copy(total, grad_any, local_sem.at[1])
        grad_copy.start()

        def drain():
            drain_sends()
            (swap(cats) if sec else swap(vals)).wait_send()
            for copy in handed + sided + passed:
                copy.wait_send()
            flow_copy.wait()
            grad_copy.wait()

        scoped("drain", drain)

    for sec in (0, 1):
        pl.when(s == sec)(functools.partial(program, sec))


def finish_kernel(micro, order_ref, flow_ref, grad_ref, out_ref, down_ref, up_ref):
    local = flow_ref.shape[0] // micro
    for slot in range(micro):
        out_ref[slot] = flow_ref[pl.ds(pl.multiple_of(order_ref[slot] * local, local), local), :]
    split = down_ref.shape[0]
    rank = down_ref.shape[1]
    for start in range(0, split, rank):
        down_ref[start:start + rank, :] = grad_ref[start:start + rank, :].T
    up_ref[...] = grad_ref[split:]


def custom_route():
    fsdp = lax.axis_size("fsdp")
    return lax.axis_size("section") == 2 and fsdp % 8 == 0 and fsdp <= 16


def run_custom(tokens, cotangent, order, value, down, out, up):
    micro, local, features = tokens.shape
    rows = micro * local
    fsdp = lax.axis_size("fsdp")
    lines, chips = fsdp // 4, fsdp // 2
    block, width = value.shape
    rank = down.shape[1]
    share_up = up.shape[0]
    both, high = width + rank, block + share_up
    plan = plan_of(width, block, share_up)
    most = max(sum(item[0] == array for item in plan) for array in (OUT, MIX))
    outside, inside = pl.BlockSpec(memory_space=pl.ANY), pl.BlockSpec(memory_space=pltpu.VMEM)
    dma = pltpu.SemaphoreType.DMA
    vmem = pltpu.VMEM
    flow, grads = pl.pallas_call(
        functools.partial(relay_kernel, lines, plan),
        out_shape=[
            jax.ShapeDtypeStruct((rows, features), bf16),
            jax.ShapeDtypeStruct((high, rank), f32),
        ],
        in_specs=[outside] * 6,
        out_specs=[outside] * 2,
        scratch_shapes=[
            vmem((2, features, both), bf16),
            vmem((2, fsdp * width, block), bf16),
            vmem((fsdp * share_up, rank), bf16),
            vmem((rows, features), bf16),
            vmem((rows, features), bf16),
            vmem((rows, features), bf16),
            vmem((rows, features), bf16),
            vmem((rows, features), f32),
            vmem((rows, features), bf16),
            vmem((rows, both), f32),
            vmem((rows, width), bf16),
            vmem((rows, both), bf16),
            vmem((rows, both), bf16),
            vmem((rows, rank), bf16),
            vmem((rows, 128), f32),
            vmem((rows, 128), f32),
            vmem((rows, 128), f32),
            vmem((2, lines, 2, high, rank), bf16),
            vmem((lines, 2, high, rank), bf16),
            vmem((lines, high, rank), bf16),
            vmem((lines, high, rank), bf16),
            vmem((lines, high, rank), bf16),
            vmem((lines, high, rank), bf16),
            vmem((high, rank), f32),
            dma((6,)),
            dma((chips * (len(plan) + most + 4),)),
            dma((12,)),
            dma((2,)),
            dma((4,)),
            dma((lines * 2,)),
            dma((lines * 2,)),
        ],
        compiler_params=pltpu.CompilerParams(
            collective_id=0, has_side_effects=True, vmem_limit_bytes=67_000_000
        ),
    )(tokens.reshape(rows, features), cotangent.reshape(rows, features), value, down, out, up)
    return pl.pallas_call(
        functools.partial(finish_kernel, micro),
        out_shape=[
            jax.ShapeDtypeStruct((micro, local, features), bf16),
            jax.ShapeDtypeStruct((block, rank), f32),
            jax.ShapeDtypeStruct((share_up, rank), f32),
        ],
        in_specs=[pl.BlockSpec(memory_space=pltpu.SMEM), inside, inside],
        out_specs=[inside] * 3,
    )(order, flow, grads)


def gather_weights(w_value, w_out, adapter_down, adapter_up):
    sections = lax.axis_size("section")

    def whole(block):
        full = lax.all_gather(block, ("section", "fsdp"), axis=0, tiled=True)
        return full.reshape(sections, -1, block.shape[1])

    joined = jnp.concatenate([w_value[0], adapter_down[0]], axis=1)
    return whole(joined), whole(w_out[0].T), whole(adapter_up[0].T)


def body(tokens, cotangent, order, w_value, w_out, adapter_down, adapter_up):
    sections = lax.axis_size("section")
    position = lax.axis_index("section")
    micro, local, features = tokens.shape
    width = w_value.shape[2]

    if custom_route():
        out, grad_down, grad_up = run_custom(
            tokens, cotangent, order, w_value[0], adapter_down[0], w_out[0], adapter_up[0].T
        )
        return (out[None], grad_down[None], grad_up.T[None])

    joined, proj, up = gather_weights(w_value, w_out, adapter_down, adapter_up)
    current = tokens.reshape(micro * local, features)
    saved = []
    for layer in range(sections):
        widened = current.astype(jnp.float32)
        inverse = lax.rsqrt(jnp.mean(widened * widened, axis=-1, keepdims=True) + epsilon)
        normed = (widened * inverse).astype(jnp.bfloat16)
        last = layer == sections - 1
        if last:
            low = widen_dot(normed, joined[layer][:, width:]).astype(jnp.bfloat16)
        else:
            both = widen_dot(normed, joined[layer])
            low = both[:, width:].astype(jnp.bfloat16)
            values = (both[:, :width] + widen_dot(low, up[layer], ((1,), (1,)))).astype(jnp.bfloat16)
        saved.append((current, normed, low, inverse))
        if not last:
            current = (widened + widen_dot(values, proj[layer], ((1,), (1,)))).astype(jnp.bfloat16)

    upstream = cotangent.reshape(micro * local, features)
    grads, d_vals, d_lows = [], [], []
    for layer in reversed(range(sections)):
        inputs, normed, low, inverse = saved[layer]
        d_values = widen_dot(upstream, proj[layer]).astype(jnp.bfloat16)
        d_low = widen_dot(d_values, up[layer]).astype(jnp.bfloat16)
        d_normed = widen_dot(
            jnp.concatenate([d_values, d_low], axis=1), joined[layer], ((1,), (1,))
        )
        widened = inputs.astype(jnp.float32)
        project = jnp.mean(d_normed * widened, axis=-1, keepdims=True)
        upstream = (
            upstream.astype(jnp.float32)
            + inverse * (d_normed - widened * inverse * inverse * project)
        ).astype(jnp.bfloat16)
        grads.insert(0, upstream)
        d_vals.insert(0, d_values)
        d_lows.insert(0, d_low)

    def mine(items):
        chosen = items[0]
        for layer in range(1, sections):
            chosen = jnp.where(position == layer, items[layer], chosen)
        return chosen

    shares = lax.axis_size("fsdp")
    normed = mine([item[1] for item in saved])
    low = mine([item[2] for item in saved])
    part_down = widen_dot(normed, mine(d_lows), ((0,), (0,)))
    part_up = widen_dot(mine(d_vals), low, ((0,), (0,)))
    rank = low.shape[1]
    parts = jnp.concatenate(
        [part_down.reshape(shares, -1, rank), part_up.reshape(shares, -1, rank)], axis=1
    )
    share_down = features // shares
    combined = lax.psum_scatter(parts, "fsdp", scatter_dimension=0, tiled=True)[0]
    grad_down, grad_up = combined[:share_down], combined[share_down:]
    out = mine(grads).reshape(micro, local, features)[order]
    return (out[None], grad_down[None], grad_up.T[None])


def solution(mesh):
    return jax.shard_map(
        body,
        mesh=mesh,
        in_specs=(
            P(None, "fsdp", None),
            P(None, "fsdp", None),
            P(),
            P("section", "fsdp", None),
            P("section", None, "fsdp"),
            P("section", "fsdp", None),
            P("section", None, "fsdp"),
        ),
        out_specs=(
            P("section", None, "fsdp", None),
            P("section", "fsdp", None),
            P("section", None, "fsdp"),
        ),
        check_vma=False,
    )
```

```python
import functools

import jax
import jax.numpy as jnp
from jax import lax
from jax.experimental import pallas as pl
from jax.experimental.pallas import tpu as pltpu
from jax.sharding import PartitionSpec as P

epsilon = 1e-05
MESH = pl.DeviceIdType.MESH
X, Y, Z = 0, 1, 2
OUT, MIX, UP = 0, 1, 2
bf16, f32 = jnp.bfloat16, jnp.float32


def widen_dot(left, right, dims=((1,), (0,))):
    return lax.dot_general(left, right, (dims, ((), ())), preferred_element_type=f32)


def plan_of(out_rows, mix_rows, up_rows):
    def cut(array, rows, shares):
        start, result = 0, []
        for share, order, late in shares:
            count = rows * share // 32
            result.append((array, start, count, order, late))
            start += count
        return result

    soon = ((-1, 0), (-1, 0))
    return tuple(
        cut(UP, up_rows, [(32, (Z, Y), soon)])
        + cut(OUT, out_rows, [
                (7, (Z, Y, X), ((-0.25, -1.0), (-0.25, 2.0))),
                (10, (Z, Y, X), ((0, 0.25), (0, 0.0))),
                (8, (Y, Z, X), ((0.5, 0), (-0.75, 1.25))),
                (7, (X, Z, Y), ((2, -1.5), (0.25, 1.75))),
            ])
        + cut(MIX, mix_rows, [
                (8, (Z, Y, X), ((-0.5, 2.5), (0.75, 1.25))),
                (16, (Z, Y, X), ((0.25, -0.5), (-1, 0.75))),
                (4, (X, Z, Y), ((0, 1.5), (1.5, 2.0))),
                (4, (X, Y, Z), ((-0.25, 2), (2, -1))),
            ])
    )


def relay_kernel(
    lines, plan, tok_any, cot_any, value_any, down_any, out_any, up_any, flow_any, grad_any,
    mix, out, up, tok, cot, normed, states, wide, flow, acc, vals, cats, tail, low, squares, products, scales,
    parts, near, mine, beside_sums, sent, far, total,
    local_sem, recv_sem, send_sem, swap_sem, near_sem, side_sem, far_sem,
):
    pieces = len(plan)
    rows, features = tok.shape
    width, rank = vals.shape[1], low.shape[1]
    fsdp, chips = lines * 4, lines * 2
    block = features // fsdp
    sheet = block * 4
    share_up = up.shape[0] // fsdp
    high = {UP: share_up, OUT: width, MIX: block}
    count_of = {array: sum(item[0] == array for item in plan) for array in high}
    lead = {array: min(index for index in range(pieces) if plan[index][0] == array) for array in high}
    kinds = pieces + max(count_of[OUT], count_of[MIX])
    s, f = lax.axis_index("section"), lax.axis_index("fsdp")
    core, y, z = f % 2, (f // 2) % 2, f // 4
    chip = f // 2

    def place(s_, z_, y_, c_):
        return {"section": s_, "fsdp": (z_ * 2 + y_) * 2 + c_}

    partner = place(s, z, y, 1 - core)
    across = place(1 - s, z, y, core)
    beside = place(s, z, 1 - y, core)
    above = place(s, z + 1, y, core)
    below = place(s, z - 1, y, core)

    def stage(source, target, index):
        copy = pltpu.make_async_copy(source, target, local_sem.at[index])
        copy.start()
        return copy

    def band(array, slot, start, count):
        return pl.ds(pl.multiple_of(slot * high[array] + start, 16), count)

    staged = {
        UP: [stage(up_any, up.at[band(UP, f, 0, share_up), :], 0)],
        OUT: [stage(out_any, out.at[s, band(OUT, f, 0, width), :], 1)],
        MIX: [
            stage(value_any, mix.at[s, band(MIX, f, 0, block), :width], 2),
            stage(down_any, mix.at[s, band(MIX, f, 0, block), width:], 3),
        ],
    }
    inputs_staged = [stage(tok_any, tok, 4), stage(cot_any, cot, 5)]

    barrier = pltpu.get_barrier_semaphore()
    for target in (partner, across, beside):
        pl.semaphore_signal(barrier, inc=1, device_id=target, device_id_type=MESH)

    @pl.when(z + 1 < lines)
    def _():
        pl.semaphore_signal(barrier, inc=1, device_id=above, device_id_type=MESH)

    @pl.when(z > 0)
    def _():
        pl.semaphore_signal(barrier, inc=1, device_id=below, device_id_type=MESH)

    ends = (z + 1 < lines).astype(jnp.int32) + (z > 0).astype(jnp.int32)
    pl.semaphore_wait(barrier, 3 + ends)
    for array in (UP, OUT, MIX):
        for copy in staged[array]:
            copy.wait()

    def when(test, action):
        if test is True:
            action()
        else:
            pl.when(test)(action)

    def both(left, right):
        return right if left is True else left if right is True else left & right

    def slot_of(dy, dz, c_):
        return ((z + dz) * 2 + (y + dy) % 2) * 2 + c_

    def held(array, owner, span):
        return up.at[span, :] if array == UP else (mix if array == MIX else out).at[owner, span, :]

    def piece(index, owner, slot):
        array, start, count = plan[index][:3]
        return held(array, owner, band(array, slot, start, count))

    def whole(array, owner, slot):
        return held(array, owner, band(array, slot, 0, high[array]))

    def inside(dz):
        return True if dz == 0 else (z + dz < lines) if dz > 0 else (z + dz >= 0)

    def sem_of(index, dx, slot):
        kind = pieces + index - lead[plan[index][0]] if dx else index
        return recv_sem.at[slot // 2 * (kinds + 4) + kind]

    def whole_sem(array, dx, slot):
        return recv_sem.at[slot // 2 * (kinds + 4) + kinds + (3 if dx else array)]

    turned = z // (lines // 2)
    folded = z + turned * (lines - 1 - 2 * z)

    def plane_of(reach):
        near_plane = folded if reach == 0 else 1 - folded if reach == 1 else reach
        return near_plane + turned * (lines - 1 - 2 * near_plane)

    def columns(index, count):
        return pl.ds(pl.multiple_of(index * count, count), count)

    def fold(product):
        sums = product[:, :128]
        for start in range(128, product.shape[1], 128):
            sums = sums + product[:, start:start + 128]
        return sums

    step = width

    def blocks(action, size=step):
        def run(index, carry):
            action(index)
            return carry

        lax.fori_loop(0, features // size, run, 0, unroll=4)

    def mean_of(sums):
        return jnp.sum(sums[...], axis=1, keepdims=True) / features

    def ups():
        return up[...]

    def block_of_out(owner, slot):
        return out[owner, band(OUT, slot, 0, width), :]

    def swap(ref):
        return pltpu.make_async_remote_copy(
            src_ref=ref,
            dst_ref=ref,
            send_sem=swap_sem.at[0],
            recv_sem=swap_sem.at[1],
            device_id=across,
            device_id_type=MESH,
        )

    acc[...] = jnp.zeros_like(acc)
    squares[...] = jnp.zeros_like(squares)
    products[...] = jnp.zeros_like(products)

    def program(sec):
        lone, common = (MIX, OUT) if sec == 0 else (OUT, MIX)

        def late(index, dx):
            return plan[index][4][sec][dx]

        def routes(index, dx, dy, dz):
            gone, result = {X: dx != 0, Y: dy != 0, Z: dz != 0}, []
            for turn, dim in enumerate(plan[index][3]):
                if any(gone[later] for later in plan[index][3][turn + 1:]):
                    continue
                if dim == Z:
                    result += [(Z, 1)] * (dz <= 0) + [(Z, -1)] * (dz >= 0)
                elif dim == Y and not gone[Y]:
                    result.append((Y, 1))
                elif dim == X and not gone[X] and plan[index][0] == common:
                    result.append((X, 1))
            return result

        def push(ref, array, way, target, sem):
            pltpu.make_async_remote_copy(
                src_ref=ref,
                dst_ref=ref,
                send_sem=send_sem.at[array * 4 + way],
                recv_sem=sem,
                device_id=target,
                device_id_type=MESH,
            ).start()

        def send_all(index, dx, dy, dz):
            slot, array = slot_of(dy, dz, core), plan[index][0]
            here = piece(index, (sec + dx) % 2, slot)
            for dim, sign in routes(index, dx, dy, dz):
                target = {Y: beside, X: across}.get(dim, above if sign > 0 else below)
                test = True if dim != Z else z + 1 < lines if sign > 0 else z > 0
                sem = sem_of(index, 1 if dim == X else dx, slot)
                when(test, functools.partial(push, here, array, dim, target, sem))

        def arrived(index, dx, slot):
            ref = piece(index, (sec + dx) % 2, slot)
            pltpu.make_async_copy(ref, ref, sem_of(index, dx, slot)).wait()

        def partners_arrived(array, dx, plane):
            for y_ in (0, 1):
                slot = (plane * 2 + y_) * 2 + 1 - core
                ref = whole(array, (sec + dx) % 2, slot)
                pltpu.make_async_copy(ref, ref, whole_sem(array, dx, slot)).wait()

        events = []
        for dx in (0, 1):
            for dy in (0, 1):
                for dz in range(1 - lines, lines):
                    for index in range(pieces):
                        if not dx or plan[index][0] == lone:
                            key = dx + dy + abs(dz) + late(index, dx)
                            events.append((key, index, dx, abs(dz), dy, dz))
        events.sort()
        closing = {(plan[index][0], dx, dy, dz): number for number, (_, index, dx, _, dy, dz) in enumerate(events)}

        def relay(number, index, dx, dy, dz):
            array, slot = plan[index][0], slot_of(dy, dz, core)

            def action():
                if dx or dy or dz:
                    arrived(index, dx, slot)
                send_all(index, dx, dy, dz)
                if closing[array, dx, dy, dz] == number:
                    push(whole(array, (sec + dx) % 2, slot), array, 3, partner, whole_sem(array, dx, slot))

            when(inside(dz), action)

        def sent_rows(array, way, z_):
            rows_ = 0
            for _, index, dx, _, dy, dz in events:
                if plan[index][0] == array and 0 <= z_ + dz < lines:
                    for dim, sign in routes(index, dx, dy, dz):
                        if dim == way and (dim != Z or 0 <= z_ + sign < lines):
                            rows_ += plan[index][2]
            if way == 3:
                rows_ = high[array] * chips * (2 if array == lone else 1)
            return rows_

        def drain_sends():
            for array in high:
                for way in (X, Y, Z, 3):
                    for fold_ in range(lines // 2):
                        rows_ = sent_rows(array, way, fold_)
                        if not rows_ or (way != Z and fold_):
                            continue

                        def wait(rows_=rows_, array=array, way=way):
                            ref = held(array, 0, pl.ds(0, rows_))
                            pltpu.make_async_copy(ref, ref, send_sem.at[array * 4 + way]).wait()

                        when(folded == fold_ if way == Z else True, wait)

        def ready(array, dx, reach):
            return max(dx + 1 + reach + late(index, dx) for index in range(pieces) if plan[index][0] == array)

        def prepare():
            for copy in inputs_staged:
                copy.wait()
            if sec:
                return

            def square(index):
                entries = tok[:, columns(index, step)].astype(f32)
                squares[...] += fold(entries * entries)

            blocks(square)
            inverse = lax.rsqrt(mean_of(squares) + epsilon)

            def scale(index):
                span = columns(index, step)
                normed[:, span] = (tok[:, span].astype(f32) * inverse).astype(bf16)

            blocks(scale)
            scales[...] = jnp.broadcast_to(inverse, scales.shape)
            squares[...] = jnp.zeros_like(squares)

        def part_of(plane, part):
            return pl.ds(pl.multiple_of(plane * sheet + part * block, block), block)

        def lone_plane(reach):
            plane = plane_of(reach)
            partners_arrived(lone, 0, plane)
            if sec == 0:
                span = columns(plane, sheet)
                acc[...] += widen_dot(normed[:, span], mix[0, span, :])
                return
            sums = acc[:, :width]
            for part in range(4):
                sums = sums + widen_dot(cot[:, part_of(plane, part)], block_of_out(1, plane * 4 + part), ((1,), (1,)))
            acc[:, :width] = sums

        def emit():
            for plane in range(lines):
                partners_arrived(UP, 0, plane)
            if sec == 0:
                low[...] = acc[:, width:].astype(bf16)
                vals[...] = (acc[:, :width] + widen_dot(low[...], ups(), ((1,), (1,)))).astype(bf16)
                swap(vals).start()
            else:
                cats[:, :width] = acc[:, :width].astype(bf16)
                cats[:, width:] = widen_dot(cats[:, :width], ups()).astype(bf16)
                swap(cats).start()

        def widen(reach):
            plane = plane_of(reach)
            partners_arrived(OUT, sec, plane)
            for part in range(4):
                span = part_of(plane, part)
                added = widen_dot(vals[...], block_of_out(0, plane * 4 + part))
                entries = (tok[:, span].astype(f32) + added).astype(bf16)
                states[:, span] = entries
                back = entries.astype(f32)
                squares[...] += fold(back * back)
                if sec:
                    products[...] += fold(back * wide[:, span])

        def open_up(layer, joint, span, inputs):
            entries = widen_dot(joint[...], mix[layer, span, :], ((1,), (1,)))
            wide[:, span] = entries
            if inputs is not None:
                products[...] += fold(entries * inputs[:, span].astype(f32))

        def open_plane(reach):
            plane = plane_of(reach)
            partners_arrived(MIX, 1 - sec, plane)
            for part in range(2):
                span = pl.ds(pl.multiple_of(plane * sheet + part * step, step), step)
                open_up(1, cats, span, states if sec == 0 else None)

        def scoped(name, action, *args):
            with jax.named_scope(name):
                action(*args)

        timeline = [(key, 0, number, "relay%d" % int(key), functools.partial(relay, number, *event[:2], *event[3:]))
                    for number, (key, *event) in enumerate(events)]
        emitted = max(ready(lone, 0, lines - 1), ready(UP, 0, lines - 1)) + 0.02
        swapped = (1000, 1000)[sec]
        timeline.append((0.01, 1, 0, "prepare", prepare))
        timeline.append((emitted, 2, 0, "emit", emit))
        for reach in range(lines):
            pause = 0.7 if reach < lines - 1 else 0
            timeline.append((ready(lone, 0, reach) + pause, 1, reach, "lone", functools.partial(lone_plane, reach)))
            early, behind = (widen, open_plane) if sec == 0 else (open_plane, widen)
            pause = 0.0 if reach < lines - 1 else 0
            key = max(ready(common, 0, reach) + pause, emitted)
            timeline.append((key, 3, reach, early.__name__, functools.partial(early, reach)))
            key = max(ready(lone, 1, reach), swapped)
            timeline.append((key, 4, reach, behind.__name__, functools.partial(behind, reach)))
        timeline.append((swapped, 3, 9, "swapped", swap(vals).wait_recv if sec else swap(cats).wait_recv))
        timeline.sort(key=lambda item: item[:3])
        for _, _, _, name, action in timeline:
            scoped(name, action)

        def gradients(joint):
            turned_low = joint[:, width:].T
            for index in range(fsdp):
                product = widen_dot(turned_low, normed[:, index * block:(index + 1) * block]).astype(bf16)
                for start in range(0, block, rank):
                    parts[index % 2, index // 4, index // 2 % 2, start:start + rank, :] = product[:, start:start + rank]
            ends = widen_dot(joint[:, :width], low[...], ((0,), (0,))).astype(bf16)
            for index in range(fsdp):
                owned = ends[index * share_up:(index + 1) * share_up]
                parts[index % 2, index // 4, index // 2 % 2, block:, :] = owned

        handed, sided, passed = [], [], []
        half = lines // 2

        def settle():
            for turn in (0, 1):
                span = pl.ds((turned + 1 + turn) % 2 * half, half)
                copy = pltpu.make_async_remote_copy(
                    src_ref=parts.at[1 - core, span],
                    dst_ref=near.at[span],
                    send_sem=near_sem.at[2 + turn],
                    recv_sem=near_sem.at[turn],
                    device_id=partner,
                    device_id_type=MESH,
                )
                copy.start()
                handed.append(copy)
            for turn in range(lines):
                if turn % half == 0:
                    handed[turn // half].wait_recv()
                plane = plane_of(lines - 1 - turn)
                mine[plane] = (parts[core, plane, 1 - y].astype(f32) + near[plane, 1 - y].astype(f32)).astype(bf16)
                copy = pltpu.make_async_remote_copy(
                    src_ref=mine.at[plane],
                    dst_ref=beside_sums.at[plane],
                    send_sem=side_sem.at[lines + turn],
                    recv_sem=side_sem.at[turn],
                    device_id=beside,
                    device_id_type=MESH,
                )
                sided.append(copy)
                if turn:
                    sided[turn - 1].start()
            sided[-1].start()

        def pass_on():
            for turn in range(lines):
                sided[turn].wait_recv()
                plane = plane_of(lines - 1 - turn)
                sums = parts[core, plane, y].astype(f32) + near[plane, y].astype(f32) + beside_sums[plane].astype(f32)
                if turn == lines - 1:
                    total[...] = sums
                    continue
                sent[turn] = sums.astype(bf16)
                copy = pltpu.make_async_remote_copy(
                    src_ref=sent.at[turn],
                    dst_ref=far.at[z],
                    send_sem=far_sem.at[lines + turn],
                    recv_sem=far_sem.at[z],
                    device_id=place(s, plane, y, core),
                    device_id_type=MESH,
                )
                copy.start()
                passed.append(copy)

        def write_flow():
            copy = pltpu.make_async_copy(flow, flow_any, local_sem.at[0])
            copy.start()
            return copy

        inverse = lax.rsqrt(mean_of(squares) + epsilon)

        def upstream_of(span, factor):
            inputs = states[:, span].astype(f32)
            entries = cot[:, span].astype(f32) + inverse * (wide[:, span] - inputs * factor)
            flow[:, span] = entries.astype(bf16)

        acc[...] = jnp.zeros_like(acc)
        factor = inverse * inverse * mean_of(products)
        if sec == 0:
            def narrow():
                sums = jnp.zeros((rows, width), f32)
                for index in range(fsdp):
                    span = slice(index * block, (index + 1) * block)
                    upstream_of(span, factor)
                    sums = sums + widen_dot(flow[:, span], out[0, index * width:(index + 1) * width, :], ((1,), (1,)))
                tail[:, :width] = sums.astype(bf16)
                tail[:, width:] = widen_dot(tail[:, :width], ups()).astype(bf16)

            scoped("narrow", narrow)
            scoped("grads", gradients, tail)
            scoped("settle", settle)
            products[...] = jnp.zeros_like(products)
            scoped("open0", blocks, lambda index: open_up(0, tail, columns(index, step), tok))
            scoped("pass", pass_on)
            first_inverse = scales[:, :1]
            first_factor = first_inverse * first_inverse * mean_of(products)

            def finish(index):
                span = columns(index, step)
                change = wide[:, span] - tok[:, span].astype(f32) * first_factor
                flow[:, span] = (flow[:, span].astype(f32) + first_inverse * change).astype(bf16)

            scoped("finish", blocks, finish)
            flow_copy = write_flow()
        else:
            def lower(index):
                span = columns(index, step)
                normed[:, span] = (states[:, span].astype(f32) * inverse).astype(bf16)
                acc[:, width:] += widen_dot(normed[:, span], mix[1, span, width:])

            scoped("lower", blocks, lower)
            low[...] = acc[:, width:].astype(bf16)
            scoped("grads", gradients, cats)
            scoped("settle", settle)
            scoped("upstream", blocks, lambda index: upstream_of(columns(index, step), factor))
            flow_copy = write_flow()
            scoped("pass", pass_on)

        def settled():
            for reach in range(1, lines):
                plane = plane_of(reach)
                pltpu.make_async_copy(far.at[plane], far.at[plane], far_sem.at[plane]).wait()
                total[...] += far[plane].astype(f32)

        scoped("settled", settled)
        grad_copy = pltpu.make_async_copy(total, grad_any, local_sem.at[1])
        grad_copy.start()

        def drain():
            drain_sends()
            (swap(cats) if sec else swap(vals)).wait_send()
            for copy in handed + sided + passed:
                copy.wait_send()
            flow_copy.wait()
            grad_copy.wait()

        scoped("drain", drain)

    for sec in (0, 1):
        pl.when(s == sec)(functools.partial(program, sec))


def finish_kernel(micro, order_ref, flow_ref, grad_ref, out_ref, down_ref, up_ref):
    local = flow_ref.shape[0] // micro
    for slot in range(micro):
        out_ref[slot] = flow_ref[pl.ds(pl.multiple_of(order_ref[slot] * local, local), local), :]
    split = down_ref.shape[0]
    rank = down_ref.shape[1]
    for start in range(0, split, rank):
        down_ref[start:start + rank, :] = grad_ref[start:start + rank, :].T
    up_ref[...] = grad_ref[split:]


def custom_route():
    fsdp = lax.axis_size("fsdp")
    return lax.axis_size("section") == 2 and fsdp % 8 == 0 and fsdp <= 16


def run_custom(tokens, cotangent, order, value, down, out, up):
    micro, local, features = tokens.shape
    rows = micro * local
    fsdp = lax.axis_size("fsdp")
    lines, chips = fsdp // 4, fsdp // 2
    block, width = value.shape
    rank = down.shape[1]
    share_up = up.shape[0]
    both, high = width + rank, block + share_up
    plan = plan_of(width, block, share_up)
    most = max(sum(item[0] == array for item in plan) for array in (OUT, MIX))
    outside, inside = pl.BlockSpec(memory_space=pl.ANY), pl.BlockSpec(memory_space=pltpu.VMEM)
    dma = pltpu.SemaphoreType.DMA
    vmem = pltpu.VMEM
    flow, grads = pl.pallas_call(
        functools.partial(relay_kernel, lines, plan),
        out_shape=[
            jax.ShapeDtypeStruct((rows, features), bf16),
            jax.ShapeDtypeStruct((high, rank), f32),
        ],
        in_specs=[outside] * 6,
        out_specs=[outside] * 2,
        scratch_shapes=[
            vmem((2, features, both), bf16),
            vmem((2, fsdp * width, block), bf16),
            vmem((fsdp * share_up, rank), bf16),
            vmem((rows, features), bf16),
            vmem((rows, features), bf16),
            vmem((rows, features), bf16),
            vmem((rows, features), bf16),
            vmem((rows, features), f32),
            vmem((rows, features), bf16),
            vmem((rows, both), f32),
            vmem((rows, width), bf16),
            vmem((rows, both), bf16),
            vmem((rows, both), bf16),
            vmem((rows, rank), bf16),
            vmem((rows, 128), f32),
            vmem((rows, 128), f32),
            vmem((rows, 128), f32),
            vmem((2, lines, 2, high, rank), bf16),
            vmem((lines, 2, high, rank), bf16),
            vmem((lines, high, rank), bf16),
            vmem((lines, high, rank), bf16),
            vmem((lines, high, rank), bf16),
            vmem((lines, high, rank), bf16),
            vmem((high, rank), f32),
            dma((6,)),
            dma((chips * (len(plan) + most + 4),)),
            dma((12,)),
            dma((2,)),
            dma((4,)),
            dma((lines * 2,)),
            dma((lines * 2,)),
        ],
        compiler_params=pltpu.CompilerParams(
            collective_id=0, has_side_effects=True, vmem_limit_bytes=67_000_000
        ),
    )(tokens.reshape(rows, features), cotangent.reshape(rows, features), value, down, out, up)
    return pl.pallas_call(
        functools.partial(finish_kernel, micro),
        out_shape=[
            jax.ShapeDtypeStruct((micro, local, features), bf16),
            jax.ShapeDtypeStruct((block, rank), f32),
            jax.ShapeDtypeStruct((share_up, rank), f32),
        ],
        in_specs=[pl.BlockSpec(memory_space=pltpu.SMEM), inside, inside],
        out_specs=[inside] * 3,
    )(order, flow, grads)


def gather_weights(w_value, w_out, adapter_down, adapter_up):
    sections = lax.axis_size("section")

    def whole(block):
        full = lax.all_gather(block, ("section", "fsdp"), axis=0, tiled=True)
        return full.reshape(sections, -1, block.shape[1])

    joined = jnp.concatenate([w_value[0], adapter_down[0]], axis=1)
    return whole(joined), whole(w_out[0].T), whole(adapter_up[0].T)


def body(tokens, cotangent, order, w_value, w_out, adapter_down, adapter_up):
    sections = lax.axis_size("section")
    position = lax.axis_index("section")
    micro, local, features = tokens.shape
    width = w_value.shape[2]

    if custom_route():
        out, grad_down, grad_up = run_custom(
            tokens, cotangent, order, w_value[0], adapter_down[0], w_out[0], adapter_up[0].T
        )
        return (out[None], grad_down[None], grad_up.T[None])

    joined, proj, up = gather_weights(w_value, w_out, adapter_down, adapter_up)
    current = tokens.reshape(micro * local, features)
    saved = []
    for layer in range(sections):
        widened = current.astype(jnp.float32)
        inverse = lax.rsqrt(jnp.mean(widened * widened, axis=-1, keepdims=True) + epsilon)
        normed = (widened * inverse).astype(jnp.bfloat16)
        last = layer == sections - 1
        if last:
            low = widen_dot(normed, joined[layer][:, width:]).astype(jnp.bfloat16)
        else:
            both = widen_dot(normed, joined[layer])
            low = both[:, width:].astype(jnp.bfloat16)
            values = (both[:, :width] + widen_dot(low, up[layer], ((1,), (1,)))).astype(jnp.bfloat16)
        saved.append((current, normed, low, inverse))
        if not last:
            current = (widened + widen_dot(values, proj[layer], ((1,), (1,)))).astype(jnp.bfloat16)

    upstream = cotangent.reshape(micro * local, features)
    grads, d_vals, d_lows = [], [], []
    for layer in reversed(range(sections)):
        inputs, normed, low, inverse = saved[layer]
        d_values = widen_dot(upstream, proj[layer]).astype(jnp.bfloat16)
        d_low = widen_dot(d_values, up[layer]).astype(jnp.bfloat16)
        d_normed = widen_dot(
            jnp.concatenate([d_values, d_low], axis=1), joined[layer], ((1,), (1,))
        )
        widened = inputs.astype(jnp.float32)
        project = jnp.mean(d_normed * widened, axis=-1, keepdims=True)
        upstream = (
            upstream.astype(jnp.float32)
            + inverse * (d_normed - widened * inverse * inverse * project)
        ).astype(jnp.bfloat16)
        grads.insert(0, upstream)
        d_vals.insert(0, d_values)
        d_lows.insert(0, d_low)

    def mine(items):
        chosen = items[0]
        for layer in range(1, sections):
            chosen = jnp.where(position == layer, items[layer], chosen)
        return chosen

    shares = lax.axis_size("fsdp")
    normed = mine([item[1] for item in saved])
    low = mine([item[2] for item in saved])
    part_down = widen_dot(normed, mine(d_lows), ((0,), (0,)))
    part_up = widen_dot(mine(d_vals), low, ((0,), (0,)))
    rank = low.shape[1]
    parts = jnp.concatenate(
        [part_down.reshape(shares, -1, rank), part_up.reshape(shares, -1, rank)], axis=1
    )
    share_down = features // shares
    combined = lax.psum_scatter(parts, "fsdp", scatter_dimension=0, tiled=True)[0]
    grad_down, grad_up = combined[:share_down], combined[share_down:]
    out = mine(grads).reshape(micro, local, features)[order]
    return (out[None], grad_down[None], grad_up.T[None])


def solution(mesh):
    return jax.shard_map(
        body,
        mesh=mesh,
        in_specs=(
            P(None, "fsdp", None),
            P(None, "fsdp", None),
            P(),
            P("section", "fsdp", None),
            P("section", None, "fsdp"),
            P("section", "fsdp", None),
            P("section", None, "fsdp"),
        ),
        out_specs=(
            P("section", None, "fsdp", None),
            P("section", "fsdp", None),
            P("section", None, "fsdp"),
        ),
        check_vma=False,
    )
```

```python
import functools

import jax
import jax.numpy as jnp
from jax import lax
from jax.experimental import pallas as pl
from jax.experimental.pallas import tpu as pltpu
from jax.sharding import PartitionSpec as P

epsilon = 1e-05
MESH = pl.DeviceIdType.MESH
X, Y, Z = 0, 1, 2
OUT, MIX, UP = 0, 1, 2
bf16, f32 = jnp.bfloat16, jnp.float32


def widen_dot(left, right, dims=((1,), (0,))):
    return lax.dot_general(left, right, (dims, ((), ())), preferred_element_type=f32)


def plan_of(out_rows, mix_rows, up_rows):
    def cut(array, rows, shares):
        start, result = 0, []
        for share, order, late in shares:
            count = rows * share // 32
            result.append((array, start, count, order, late))
            start += count
        return result

    soon = ((-1, 0, -1), (-1, 0, -1))
    return tuple(
        cut(UP, up_rows, [(32, (Z, Y), soon)])
        + cut(OUT, out_rows, [
                (15, (Z, Y, X), ((-0.25, 0.5, 0.25), (-0.25, -0.75, -1))),
                (9, (Y, Z, X), ((1.25, 0.25, -0.25), (-1, 2.5, -6.5))),
                (8, (X, Z, Y), ((2.0, -0.25, -1.75), (-1.25, 1.5, -2.25))),
            ])
        + cut(MIX, mix_rows, [
                (10, (Z, Y, X), ((0.0, 2.5, -0.75), (0.5, 0.5, -0.25))),
                (16, (Z, Y, X), ((0.25, -0.75, 0.25), (-2.0, -0.25, -3.0))),
                (2, (X, Z, Y), ((0.25, 0.75, 0.25), (1.5, 1.5, 1.25))),
                (4, (X, Y, Z), ((-0.75, 2.0, -0.75), (2, -2.0, 0.75))),
            ])
    )


def relay_kernel(
    lines, plan, tok_any, cot_any, value_any, down_any, out_any, up_any, flow_any, grad_any,
    mix, out, up, tok, cot, normed, states, wide, flow, acc, vals, cats, tail, low, squares, products, scales,
    parts, near, mine, beside_sums, sent, far, total,
    local_sem, recv_sem, send_sem, swap_sem, near_sem, side_sem, far_sem,
):
    pieces = len(plan)
    rows, features = tok.shape
    width, rank = vals.shape[1], low.shape[1]
    fsdp, chips = lines * 4, lines * 2
    block = features // fsdp
    sheet = block * 4
    share_up = up.shape[0] // fsdp
    high = {UP: share_up, OUT: width, MIX: block}
    count_of = {array: sum(item[0] == array for item in plan) for array in high}
    lead = {array: min(index for index in range(pieces) if plan[index][0] == array) for array in high}
    kinds = pieces + max(count_of[OUT], count_of[MIX])
    s, f = lax.axis_index("section"), lax.axis_index("fsdp")
    core, y, z = f % 2, (f // 2) % 2, f // 4
    chip = f // 2

    def place(s_, z_, y_, c_):
        return {"section": s_, "fsdp": (z_ * 2 + y_) * 2 + c_}

    partner = place(s, z, y, 1 - core)
    across = place(1 - s, z, y, core)
    beside = place(s, z, 1 - y, core)
    above = place(s, z + 1, y, core)
    below = place(s, z - 1, y, core)

    def stage(source, target, index):
        copy = pltpu.make_async_copy(source, target, local_sem.at[index])
        copy.start()
        return copy

    def band(array, slot, start, count):
        return pl.ds(pl.multiple_of(slot * high[array] + start, 16), count)

    staged = {
        UP: [stage(up_any, up.at[band(UP, f, 0, share_up), :], 0)],
        OUT: [stage(out_any, out.at[s, band(OUT, f, 0, width), :], 1)],
        MIX: [
            stage(value_any, mix.at[s, band(MIX, f, 0, block), :width], 2),
            stage(down_any, mix.at[s, band(MIX, f, 0, block), width:], 3),
        ],
    }
    inputs_staged = [stage(tok_any, tok, 4), stage(cot_any, cot, 5)]

    barrier = pltpu.get_barrier_semaphore()
    for target in (partner, across, beside):
        pl.semaphore_signal(barrier, inc=1, device_id=target, device_id_type=MESH)

    @pl.when(z + 1 < lines)
    def _():
        pl.semaphore_signal(barrier, inc=1, device_id=above, device_id_type=MESH)

    @pl.when(z > 0)
    def _():
        pl.semaphore_signal(barrier, inc=1, device_id=below, device_id_type=MESH)

    ends = (z + 1 < lines).astype(jnp.int32) + (z > 0).astype(jnp.int32)
    pl.semaphore_wait(barrier, 3 + ends)
    for array in (UP, OUT, MIX):
        for copy in staged[array]:
            copy.wait()

    def when(test, action):
        if test is True:
            action()
        else:
            pl.when(test)(action)

    def both(left, right):
        return right if left is True else left if right is True else left & right

    def slot_of(dy, dz, c_):
        return ((z + dz) * 2 + (y + dy) % 2) * 2 + c_

    def held(array, owner, span):
        return up.at[span, :] if array == UP else (mix if array == MIX else out).at[owner, span, :]

    def piece(index, owner, slot):
        array, start, count = plan[index][:3]
        return held(array, owner, band(array, slot, start, count))

    def whole(array, owner, slot):
        return held(array, owner, band(array, slot, 0, high[array]))

    def inside(dz):
        return True if dz == 0 else (z + dz < lines) if dz > 0 else (z + dz >= 0)

    def sem_of(index, dx, slot):
        kind = pieces + index - lead[plan[index][0]] if dx else index
        return recv_sem.at[slot // 2 * (kinds + 4) + kind]

    def whole_sem(array, dx, slot):
        return recv_sem.at[slot // 2 * (kinds + 4) + kinds + (3 if dx else array)]

    turned = z // (lines // 2)
    folded = z + turned * (lines - 1 - 2 * z)

    def plane_of(reach):
        near_plane = folded if reach == 0 else 1 - folded if reach == 1 else reach
        return near_plane + turned * (lines - 1 - 2 * near_plane)

    def columns(index, count):
        return pl.ds(pl.multiple_of(index * count, count), count)

    def fold(product):
        sums = product[:, :128]
        for start in range(128, product.shape[1], 128):
            sums = sums + product[:, start:start + 128]
        return sums

    step = width

    def blocks(action, size=step):
        def run(index, carry):
            action(index)
            return carry

        lax.fori_loop(0, features // size, run, 0, unroll=4)

    def mean_of(sums):
        return jnp.sum(sums[...], axis=1, keepdims=True) / features

    def ups():
        return up[...]

    def block_of_out(owner, slot):
        return out[owner, band(OUT, slot, 0, width), :]

    def swap(ref):
        return pltpu.make_async_remote_copy(
            src_ref=ref,
            dst_ref=ref,
            send_sem=swap_sem.at[0],
            recv_sem=swap_sem.at[1],
            device_id=across,
            device_id_type=MESH,
        )

    acc[...] = jnp.zeros_like(acc)
    squares[...] = jnp.zeros_like(squares)
    products[...] = jnp.zeros_like(products)

    def program(sec):
        lone, common = (MIX, OUT) if sec == 0 else (OUT, MIX)

        def late(index, dx):
            return plan[index][4][sec][dx]

        def key_of(index, dx, dy, dz):
            reach = dx + dy + abs(dz)
            return reach + plan[index][4][sec][dx if reach else 2]

        def routes(index, dx, dy, dz):
            gone, result = {X: dx != 0, Y: dy != 0, Z: dz != 0}, []
            for turn, dim in enumerate(plan[index][3]):
                if any(gone[later] for later in plan[index][3][turn + 1:]):
                    continue
                if dim == Z:
                    result += [(Z, 1)] * (dz <= 0) + [(Z, -1)] * (dz >= 0)
                elif dim == Y and not gone[Y]:
                    result.append((Y, 1))
                elif dim == X and not gone[X] and plan[index][0] == common:
                    result.append((X, 1))
            return result

        def push(ref, array, way, target, sem):
            pltpu.make_async_remote_copy(
                src_ref=ref,
                dst_ref=ref,
                send_sem=send_sem.at[array * 4 + way],
                recv_sem=sem,
                device_id=target,
                device_id_type=MESH,
            ).start()

        def send_all(index, dx, dy, dz, dims=(X, Y, Z)):
            slot, array = slot_of(dy, dz, core), plan[index][0]
            here = piece(index, (sec + dx) % 2, slot)
            for dim, sign in routes(index, dx, dy, dz):
                if dim not in dims:
                    continue
                target = {Y: beside, X: across}.get(dim, above if sign > 0 else below)
                test = True if dim != Z else z + 1 < lines if sign > 0 else z > 0
                sem = sem_of(index, 1 if dim == X else dx, slot)
                when(test, functools.partial(push, here, array, dim, target, sem))

        def arrived(index, dx, slot):
            ref = piece(index, (sec + dx) % 2, slot)
            pltpu.make_async_copy(ref, ref, sem_of(index, dx, slot)).wait()

        def partners_arrived(array, dx, plane):
            for y_ in (0, 1):
                slot = (plane * 2 + y_) * 2 + 1 - core
                ref = whole(array, (sec + dx) % 2, slot)
                pltpu.make_async_copy(ref, ref, whole_sem(array, dx, slot)).wait()

        events = []
        for dx in (0, 1):
            for dy in (0, 1):
                for dz in range(1 - lines, lines):
                    for index in range(pieces):
                        if not dx or plan[index][0] == lone:
                            events.append((key_of(index, dx, dy, dz), index, dx, abs(dz), dy, dz))
        events.sort()
        closing = {(plan[index][0], dx, dy, dz): number for number, (_, index, dx, _, dy, dz) in enumerate(events)}

        def relay(number, index, dx, dy, dz):
            array, slot = plan[index][0], slot_of(dy, dz, core)

            def action():
                if dx or dy or dz:
                    arrived(index, dx, slot)
                    send_all(index, dx, dy, dz)
                else:
                    send_all(index, dx, dy, dz, (Y, Z))
                if closing[array, dx, dy, dz] == number:
                    push(whole(array, (sec + dx) % 2, slot), array, 3, partner, whole_sem(array, dx, slot))

            when(inside(dz), action)

        def sent_rows(array, way, z_):
            rows_ = 0
            for _, index, dx, _, dy, dz in events:
                if plan[index][0] == array and 0 <= z_ + dz < lines:
                    for dim, sign in routes(index, dx, dy, dz):
                        if dim == way and (dim != Z or 0 <= z_ + sign < lines):
                            rows_ += plan[index][2]
            if way == 3:
                rows_ = high[array] * chips * (2 if array == lone else 1)
            return rows_

        def drain_sends():
            for array in high:
                for way in (X, Y, Z, 3):
                    for fold_ in range(lines // 2):
                        rows_ = sent_rows(array, way, fold_)
                        if not rows_ or (way != Z and fold_):
                            continue

                        def wait(rows_=rows_, array=array, way=way):
                            ref = held(array, 0, pl.ds(0, rows_))
                            pltpu.make_async_copy(ref, ref, send_sem.at[array * 4 + way]).wait()

                        when(folded == fold_ if way == Z else True, wait)

        def ready(array, dx, reach):
            keys = [
                max(dx + 1 + reach + late(index, dx), plan[index][4][sec][2 * (not dx)])
                for index in range(pieces) if plan[index][0] == array
            ]
            return max(keys)

        def prepare():
            for copy in inputs_staged:
                copy.wait()
            if sec:
                return

            def square(index):
                entries = tok[:, columns(index, step)].astype(f32)
                squares[...] += fold(entries * entries)

            blocks(square)
            inverse = lax.rsqrt(mean_of(squares) + epsilon)

            def scale(index):
                span = columns(index, step)
                normed[:, span] = (tok[:, span].astype(f32) * inverse).astype(bf16)

            blocks(scale)
            scales[...] = jnp.broadcast_to(inverse, scales.shape)
            squares[...] = jnp.zeros_like(squares)

        def part_of(plane, part):
            return pl.ds(pl.multiple_of(plane * sheet + part * block, block), block)

        def lone_plane(reach):
            plane = plane_of(reach)
            partners_arrived(lone, 0, plane)
            if sec == 0:
                span = columns(plane, sheet)
                acc[...] += widen_dot(normed[:, span], mix[0, span, :])
                return
            sums = acc[:, :width]
            for part in range(4):
                sums = sums + widen_dot(cot[:, part_of(plane, part)], block_of_out(1, plane * 4 + part), ((1,), (1,)))
            acc[:, :width] = sums

        def emit():
            for plane in range(lines):
                partners_arrived(UP, 0, plane)
            if sec == 0:
                low[...] = acc[:, width:].astype(bf16)
                vals[...] = (acc[:, :width] + widen_dot(low[...], ups(), ((1,), (1,)))).astype(bf16)
                swap(vals).start()
            else:
                cats[:, :width] = acc[:, :width].astype(bf16)
                cats[:, width:] = widen_dot(cats[:, :width], ups()).astype(bf16)
                swap(cats).start()

        def widen(reach):
            plane = plane_of(reach)
            partners_arrived(OUT, sec, plane)
            for part in range(4):
                span = part_of(plane, part)
                added = widen_dot(vals[...], block_of_out(0, plane * 4 + part))
                entries = (tok[:, span].astype(f32) + added).astype(bf16)
                states[:, span] = entries
                back = entries.astype(f32)
                squares[...] += fold(back * back)
                if sec:
                    products[...] += fold(back * wide[:, span])

        def open_up(layer, joint, span, inputs):
            entries = widen_dot(joint[...], mix[layer, span, :], ((1,), (1,)))
            wide[:, span] = entries
            products[...] += fold(entries * inputs[:, span].astype(f32))

        def open_planes(*reaches):
            planes = [plane_of(reach) for reach in reaches]
            for plane in planes:
                partners_arrived(MIX, 1 - sec, plane)
            sums = products[...]
            for plane in planes:
                for part in range(2):
                    span = pl.ds(pl.multiple_of(plane * sheet + part * step, step), step)
                    entries = widen_dot(cats[...], mix[1, span, :], ((1,), (1,)))
                    wide[:, span] = entries
                    if sec == 0:
                        sums = sums + fold(entries * states[:, span].astype(f32))
            products[...] = sums

        def scoped(name, action, *args):
            with jax.named_scope(name):
                action(*args)

        timeline = [(key, 0, number, "relay%d" % int(key), functools.partial(relay, number, *event[:2], *event[3:]))
                    for number, (key, *event) in enumerate(events)]
        emitted = max(ready(lone, 0, lines - 1), ready(UP, 0, lines - 1)) + 0.02
        timeline.append((0.01, 1, 0, "prepare", prepare))
        timeline.append((emitted, 2, 0, "emit", emit))
        for reach in range(lines):
            timeline.append((ready(lone, 0, reach), 1, reach, "lone", functools.partial(lone_plane, reach)))
            key = max(ready(common, 0, reach), emitted)
            if sec == 0:
                timeline.append((key, 3, reach, "widen", functools.partial(widen, reach)))
            else:
                timeline.append((key, 3, reach, "open", functools.partial(open_planes, reach)))
                timeline.append((1000, 4, reach, "widen", functools.partial(widen, reach)))
        if sec == 0:
            timeline.append((1000, 4, 0, "open", functools.partial(open_planes, *range(lines - 1))))
            timeline.append((1000, 4, 1, "open", functools.partial(open_planes, lines - 1)))
        timeline.append((1000, 3, 0, "swapped", swap(vals).wait_recv if sec else swap(cats).wait_recv))
        timeline.sort(key=lambda item: item[:3])
        for index in range(pieces):
            send_all(index, 0, 0, 0, (X,))
        for _, _, _, name, action in timeline:
            scoped(name, action)

        handed, sided, passed = [], [], []

        def settle(joint):
            turned_low = joint[:, width:].T
            for turn in range(lines):
                plane = plane_of(lines - 1 - turn)
                ends = widen_dot(joint[:, columns(plane, share_up * 4)], low[...], ((0,), (0,))).astype(bf16)
                for part in range(4):
                    product = widen_dot(turned_low, normed[:, part_of(plane, part)]).astype(bf16)
                    for start in range(0, block, rank):
                        parts[part % 2, plane, part // 2, start:start + rank, :] = product[:, start:start + rank]
                    parts[part % 2, plane, part // 2, block:, :] = ends[part * share_up:(part + 1) * share_up]
                copy = pltpu.make_async_remote_copy(
                    src_ref=parts.at[1 - core, plane],
                    dst_ref=near.at[plane],
                    send_sem=near_sem.at[lines + turn],
                    recv_sem=near_sem.at[turn],
                    device_id=partner,
                    device_id_type=MESH,
                )
                handed.append(copy)
                if turn:
                    handed[turn - 1].start()
            handed[-1].start()
            for turn in range(lines):
                handed[turn].wait_recv()
                plane = plane_of(lines - 1 - turn)
                mine[plane] = (parts[core, plane, 1 - y].astype(f32) + near[plane, 1 - y].astype(f32)).astype(bf16)
                copy = pltpu.make_async_remote_copy(
                    src_ref=mine.at[plane],
                    dst_ref=beside_sums.at[plane],
                    send_sem=side_sem.at[lines + turn],
                    recv_sem=side_sem.at[turn],
                    device_id=beside,
                    device_id_type=MESH,
                )
                sided.append(copy)
                if turn:
                    sided[turn - 1].start()
            sided[-1].start()

        def pass_on():
            for turn in range(lines):
                sided[turn].wait_recv()
                plane = plane_of(lines - 1 - turn)
                sums = parts[core, plane, y].astype(f32) + near[plane, y].astype(f32) + beside_sums[plane].astype(f32)
                if turn == lines - 1:
                    total[...] = sums
                    continue
                sent[turn] = sums.astype(bf16)
                copy = pltpu.make_async_remote_copy(
                    src_ref=sent.at[turn],
                    dst_ref=far.at[z],
                    send_sem=far_sem.at[lines + turn],
                    recv_sem=far_sem.at[z],
                    device_id=place(s, plane, y, core),
                    device_id_type=MESH,
                )
                copy.start()
                passed.append(copy)

        def write_flow():
            copy = pltpu.make_async_copy(flow, flow_any, local_sem.at[0])
            copy.start()
            return copy

        inverse = lax.rsqrt(mean_of(squares) + epsilon)

        def upstream_of(span, factor):
            inputs = states[:, span].astype(f32)
            entries = cot[:, span].astype(f32) + inverse * (wide[:, span] - inputs * factor)
            flow[:, span] = entries.astype(bf16)

        acc[...] = jnp.zeros_like(acc)
        factor = inverse * inverse * mean_of(products)
        if sec == 0:
            def narrow():
                sums = jnp.zeros((rows, width), f32)
                for index in range(fsdp):
                    span = slice(index * block, (index + 1) * block)
                    upstream_of(span, factor)
                    sums = sums + widen_dot(flow[:, span], out[0, index * width:(index + 1) * width, :], ((1,), (1,)))
                tail[:, :width] = sums.astype(bf16)
                tail[:, width:] = widen_dot(tail[:, :width], ups()).astype(bf16)

            scoped("narrow", narrow)
            scoped("settle", settle, tail)
            products[...] = jnp.zeros_like(products)
            scoped("open0", blocks, lambda index: open_up(0, tail, columns(index, step), tok))
            first_inverse = scales[:, :1]
            first_factor = first_inverse * first_inverse * mean_of(products)

            def finish(index):
                span = columns(index, step)
                change = wide[:, span] - tok[:, span].astype(f32) * first_factor
                flow[:, span] = (flow[:, span].astype(f32) + first_inverse * change).astype(bf16)

            scoped("finish", blocks, finish)
            flow_copy = write_flow()
            scoped("pass", pass_on)
        else:
            def lower(index):
                span = columns(index, step)
                normed[:, span] = (states[:, span].astype(f32) * inverse).astype(bf16)
                acc[:, width:] += widen_dot(normed[:, span], mix[1, span, width:])

            scoped("lower", blocks, lower)
            low[...] = acc[:, width:].astype(bf16)
            scoped("settle", settle, cats)
            scoped("upstream", blocks, lambda index: upstream_of(columns(index, step), factor))
            flow_copy = write_flow()
            scoped("pass", pass_on)

        def settled():
            for reach in range(1, lines):
                plane = plane_of(reach)
                pltpu.make_async_copy(far.at[plane], far.at[plane], far_sem.at[plane]).wait()
                total[...] += far[plane].astype(f32)

        scoped("settled", settled)
        grad_copy = pltpu.make_async_copy(total, grad_any, local_sem.at[1])
        grad_copy.start()

        def drain():
            drain_sends()
            (swap(cats) if sec else swap(vals)).wait_send()
            for copy in handed + sided + passed:
                copy.wait_send()
            flow_copy.wait()
            grad_copy.wait()

        scoped("drain", drain)

    for sec in (0, 1):
        pl.when(s == sec)(functools.partial(program, sec))


def finish_kernel(micro, order_ref, flow_ref, grad_ref, out_ref, down_ref, up_ref):
    local = flow_ref.shape[0] // micro
    for slot in range(micro):
        out_ref[slot] = flow_ref[pl.ds(pl.multiple_of(order_ref[slot] * local, local), local), :]
    split = down_ref.shape[0]
    rank = down_ref.shape[1]
    for start in range(0, split, rank):
        down_ref[start:start + rank, :] = grad_ref[start:start + rank, :].T
    up_ref[...] = grad_ref[split:]


def custom_route():
    fsdp = lax.axis_size("fsdp")
    return lax.axis_size("section") == 2 and fsdp % 8 == 0 and fsdp <= 16


def run_custom(tokens, cotangent, order, value, down, out, up):
    micro, local, features = tokens.shape
    rows = micro * local
    fsdp = lax.axis_size("fsdp")
    lines, chips = fsdp // 4, fsdp // 2
    block, width = value.shape
    rank = down.shape[1]
    share_up = up.shape[0]
    both, high = width + rank, block + share_up
    plan = plan_of(width, block, share_up)
    most = max(sum(item[0] == array for item in plan) for array in (OUT, MIX))
    outside, inside = pl.BlockSpec(memory_space=pl.ANY), pl.BlockSpec(memory_space=pltpu.VMEM)
    dma = pltpu.SemaphoreType.DMA
    vmem = pltpu.VMEM
    flow, grads = pl.pallas_call(
        functools.partial(relay_kernel, lines, plan),
        out_shape=[
            jax.ShapeDtypeStruct((rows, features), bf16),
            jax.ShapeDtypeStruct((high, rank), f32),
        ],
        in_specs=[outside] * 6,
        out_specs=[outside] * 2,
        scratch_shapes=[
            vmem((2, features, both), bf16),
            vmem((2, fsdp * width, block), bf16),
            vmem((fsdp * share_up, rank), bf16),
            vmem((rows, features), bf16),
            vmem((rows, features), bf16),
            vmem((rows, features), bf16),
            vmem((rows, features), bf16),
            vmem((rows, features), f32),
            vmem((rows, features), bf16),
            vmem((rows, both), f32),
            vmem((rows, width), bf16),
            vmem((rows, both), bf16),
            vmem((rows, both), bf16),
            vmem((rows, rank), bf16),
            vmem((rows, 128), f32),
            vmem((rows, 128), f32),
            vmem((rows, 128), f32),
            vmem((2, lines, 2, high, rank), bf16),
            vmem((lines, 2, high, rank), bf16),
            vmem((lines, high, rank), bf16),
            vmem((lines, high, rank), bf16),
            vmem((lines, high, rank), bf16),
            vmem((lines, high, rank), bf16),
            vmem((high, rank), f32),
            dma((6,)),
            dma((chips * (len(plan) + most + 4),)),
            dma((12,)),
            dma((2,)),
            dma((lines * 2,)),
            dma((lines * 2,)),
            dma((lines * 2,)),
        ],
        compiler_params=pltpu.CompilerParams(
            collective_id=0, has_side_effects=True, vmem_limit_bytes=67_000_000
        ),
    )(tokens.reshape(rows, features), cotangent.reshape(rows, features), value, down, out, up)
    return pl.pallas_call(
        functools.partial(finish_kernel, micro),
        out_shape=[
            jax.ShapeDtypeStruct((micro, local, features), bf16),
            jax.ShapeDtypeStruct((block, rank), f32),
            jax.ShapeDtypeStruct((share_up, rank), f32),
        ],
        in_specs=[pl.BlockSpec(memory_space=pltpu.SMEM), inside, inside],
        out_specs=[inside] * 3,
    )(order, flow, grads)


def gather_weights(w_value, w_out, adapter_down, adapter_up):
    sections = lax.axis_size("section")

    def whole(block):
        full = lax.all_gather(block, ("section", "fsdp"), axis=0, tiled=True)
        return full.reshape(sections, -1, block.shape[1])

    joined = jnp.concatenate([w_value[0], adapter_down[0]], axis=1)
    return whole(joined), whole(w_out[0].T), whole(adapter_up[0].T)


def body(tokens, cotangent, order, w_value, w_out, adapter_down, adapter_up):
    sections = lax.axis_size("section")
    position = lax.axis_index("section")
    micro, local, features = tokens.shape
    width = w_value.shape[2]

    if custom_route():
        out, grad_down, grad_up = run_custom(
            tokens, cotangent, order, w_value[0], adapter_down[0], w_out[0], adapter_up[0].T
        )
        return (out[None], grad_down[None], grad_up.T[None])

    joined, proj, up = gather_weights(w_value, w_out, adapter_down, adapter_up)
    current = tokens.reshape(micro * local, features)
    saved = []
    for layer in range(sections):
        widened = current.astype(jnp.float32)
        inverse = lax.rsqrt(jnp.mean(widened * widened, axis=-1, keepdims=True) + epsilon)
        normed = (widened * inverse).astype(jnp.bfloat16)
        last = layer == sections - 1
        if last:
            low = widen_dot(normed, joined[layer][:, width:]).astype(jnp.bfloat16)
        else:
            both = widen_dot(normed, joined[layer])
            low = both[:, width:].astype(jnp.bfloat16)
            values = (both[:, :width] + widen_dot(low, up[layer], ((1,), (1,)))).astype(jnp.bfloat16)
        saved.append((current, normed, low, inverse))
        if not last:
            current = (widened + widen_dot(values, proj[layer], ((1,), (1,)))).astype(jnp.bfloat16)

    upstream = cotangent.reshape(micro * local, features)
    grads, d_vals, d_lows = [], [], []
    for layer in reversed(range(sections)):
        inputs, normed, low, inverse = saved[layer]
        d_values = widen_dot(upstream, proj[layer]).astype(jnp.bfloat16)
        d_low = widen_dot(d_values, up[layer]).astype(jnp.bfloat16)
        d_normed = widen_dot(
            jnp.concatenate([d_values, d_low], axis=1), joined[layer], ((1,), (1,))
        )
        widened = inputs.astype(jnp.float32)
        project = jnp.mean(d_normed * widened, axis=-1, keepdims=True)
        upstream = (
            upstream.astype(jnp.float32)
            + inverse * (d_normed - widened * inverse * inverse * project)
        ).astype(jnp.bfloat16)
        grads.insert(0, upstream)
        d_vals.insert(0, d_values)
        d_lows.insert(0, d_low)

    def mine(items):
        chosen = items[0]
        for layer in range(1, sections):
            chosen = jnp.where(position == layer, items[layer], chosen)
        return chosen

    shares = lax.axis_size("fsdp")
    normed = mine([item[1] for item in saved])
    low = mine([item[2] for item in saved])
    part_down = widen_dot(normed, mine(d_lows), ((0,), (0,)))
    part_up = widen_dot(mine(d_vals), low, ((0,), (0,)))
    rank = low.shape[1]
    parts = jnp.concatenate(
        [part_down.reshape(shares, -1, rank), part_up.reshape(shares, -1, rank)], axis=1
    )
    share_down = features // shares
    combined = lax.psum_scatter(parts, "fsdp", scatter_dimension=0, tiled=True)[0]
    grad_down, grad_up = combined[:share_down], combined[share_down:]
    out = mine(grads).reshape(micro, local, features)[order]
    return (out[None], grad_down[None], grad_up.T[None])


def solution(mesh):
    return jax.shard_map(
        body,
        mesh=mesh,
        in_specs=(
            P(None, "fsdp", None),
            P(None, "fsdp", None),
            P(),
            P("section", "fsdp", None),
            P("section", None, "fsdp"),
            P("section", "fsdp", None),
            P("section", None, "fsdp"),
        ),
        out_specs=(
            P("section", None, "fsdp", None),
            P("section", "fsdp", None),
            P("section", None, "fsdp"),
        ),
        check_vma=False,
    )
```
